8 devices in a mesh: dp: 1 (over z), ep2: 2 (over y), ep: 4 (over x, core).
Axes of the slice: x: 2, y: 2, z: 1, core: 2. Of those that a mesh axis runs over, the one named last changes fastest.
Arguments:
- x_tok: bfloat16 [16384, 768], P(('dp', 'ep2', 'ep'))
- expert_ids: int32 [16384, 1], P(('dp', 'ep2', 'ep'))
- gate_w: float32 [16384, 1], P(('dp', 'ep2', 'ep'))
- w_in: bfloat16 [128, 768, 3072], P(('ep2', 'ep'))
- w_out: bfloat16 [128, 3072, 768], P(('ep2', 'ep'))
Outputs:
- output: bfloat16 [16384, 768], P(('dp', 'ep2', 'ep'))
All inputs are finite; a program needn't handle non-finite values.
Results may differ from the reference program's by a relative error of at most 0.001.
Values are sent between devices in bfloat16 or wider.
A program may use at most 1 GiB of HBM per device.

```python
import math
import jax
import jax.numpy as jnp
from jax import lax

TOKENS = 2048
GROUP = 8
D_MODEL = 768
FF = 3072
EXPERTS = 128
TOP = 1
CAP = 160


def draw_routing(route_key):
    k_perm, k_shift, k_tok, k_roll = jax.random.split(route_key, 4)
    avg_count = TOKENS * TOP // EXPERTS
    spread = avg_count - 1
    rank_of = jax.random.permutation(k_perm, EXPERTS)
    shifts = jax.random.randint(k_shift, (GROUP, 1), 0, EXPERTS // 16 + 2)
    prof_pos = (rank_of[None, :] + shifts) % EXPERTS
    near_end = jnp.minimum(prof_pos, EXPERTS - 1 - prof_pos)
    step_mag = (spread * (EXPERTS - 1 - 2 * near_end)) // (EXPERTS - 1)
    dev_counts = avg_count + jnp.where(prof_pos < EXPERTS - 1 - prof_pos, step_mag, -step_mag)
    run_end = jnp.cumsum(dev_counts, axis=1)
    list_pos = jnp.arange(TOKENS * TOP)
    sorted_ids = jax.vmap(lambda end_row: jnp.searchsorted(end_row, list_pos, side='right'))(run_end)
    id_grid = jnp.swapaxes(sorted_ids.reshape(GROUP, TOP, TOKENS), 1, 2)
    tok_keys = jax.random.split(k_tok, GROUP)
    tok_perm = jax.vmap(lambda tok_key: jax.random.permutation(tok_key, TOKENS))(tok_keys)
    id_grid = jnp.take_along_axis(id_grid, jnp.broadcast_to(tok_perm[:, :, None], (GROUP, TOKENS, TOP)), axis=1)
    roll_by = jax.random.randint(k_roll, (GROUP, TOKENS, 1), 0, TOP)
    col_ids = (jnp.arange(TOP)[None, None, :] + roll_by) % TOP
    id_grid = jnp.take_along_axis(id_grid, col_ids, axis=2)
    return id_grid.reshape(GROUP * TOKENS, TOP).astype(jnp.int32)


def setup_inputs(seed: int = 0, part: int = 0) -> dict:
    key_part = jax.random.fold_in(jax.random.key(seed), part)
    k_x, k_gate, k_route = jax.random.split(key_part, 3)
    k_in, k_out = jax.random.split(jax.random.key(seed + 1), 2)
    x_tok = jax.random.normal(k_x, (GROUP * TOKENS, D_MODEL), jnp.float32).astype(jnp.bfloat16)
    gate_w = jax.random.uniform(k_gate, (GROUP * TOKENS, TOP), jnp.float32, 0.5, 1.5) * (2.0 / math.sqrt(TOP))
    w_in = (jax.random.normal(k_in, (EXPERTS, D_MODEL, FF), jnp.float32) * (D_MODEL ** -0.5)).astype(jnp.bfloat16)
    w_out = (jax.random.normal(k_out, (EXPERTS, FF, D_MODEL), jnp.float32) * (FF ** -0.5)).astype(jnp.bfloat16)
    return {'x_tok': x_tok, 'expert_ids': draw_routing(k_route), 'gate_w': gate_w, 'w_in': w_in, 'w_out': w_out}


def reference(x_tok, expert_ids, gate_w, w_in, w_out):
    flat_e = expert_ids.reshape(-1)
    n_pair = flat_e.shape[0]
    pair_order = jnp.argsort(flat_e, stable=True)
    counts = jnp.bincount(flat_e, length=EXPERTS)
    starts = jnp.cumsum(counts) - counts
    slot_ids = jnp.arange(CAP)
    flat_gate = gate_w.reshape(-1)

    def one_expert(acc_y, inputs):
        start_at, n_count, w_a, w_b = inputs
        pair_ids = pair_order[jnp.minimum(start_at + slot_ids, n_pair - 1)]
        is_kept = slot_ids < jnp.minimum(n_count, CAP)
        tok_ids = pair_ids // TOP
        tok_rows = jnp.where(is_kept[:, None], x_tok[tok_ids], jnp.zeros((), x_tok.dtype))
        hidden = jax.nn.gelu(jnp.dot(tok_rows, w_a, preferred_element_type=jnp.float32), approximate=True).astype(jnp.bfloat16)
        out_rows = jnp.dot(hidden, w_b, preferred_element_type=jnp.float32).astype(jnp.bfloat16)
        weight = jnp.where(is_kept, flat_gate[pair_ids], 0.0)
        acc_y = acc_y.at[tok_ids].add(weight[:, None] * out_rows.astype(jnp.float32))
        return acc_y, None

    acc_y, _ = lax.scan(one_expert, x_tok.astype(jnp.float32), (starts, counts, w_in, w_out))
    return acc_y.astype(jnp.bfloat16)
```

```python
import functools

import jax
import jax.numpy as jnp
from jax import lax
from jax.experimental import pallas as pl
from jax.experimental.pallas import tpu as pltpu
from jax.sharding import PartitionSpec as P

MESH = pl.DeviceIdType.MESH
F32 = jnp.float32
BF16 = jnp.bfloat16
GROUP = 8
SPAN = 640
ZROWS = 48
FTILE = 1536


class Plan:
    def __init__(self, chunks, slots, need, need_lo, free, free_lo):
        self.chunks, self.slots = chunks, slots
        self.need, self.need_lo, self.free, self.free_lo = need, need_lo, free, free_lo
        for g in range(4):
            assert need_lo(g) == (need(g - 1) if g else 0)
            assert free_lo(g) == (free(g - 1) if g else 0)
            assert free(g) == chunks - (need(2 - g) if g < 3 else 0)
        assert need(3) == chunks

    def caps(self):
        return [self.need(g) * ZROWS for g in range(4)]


PLANS = (
    Plan(7, 4, lambda g: 3 + g + g // 2, lambda g: 2 * ((g + 2) // 3) + g + g // 3,
         lambda g: 1 + 2 * g - g // 2 + g // 3, lambda g: g + g // 2),
    Plan(8, 4, lambda g: 3 + 2 * g - g // 3, lambda g: 2 * g + (g + 2) // 3,
         lambda g: 1 + 2 * g + g // 3, lambda g: 2 * g - (g + 2) // 3),
    Plan(11, 3, lambda g: 3 + 3 * g - g // 2, lambda g: 3 * g - g // 3,
         lambda g: 3 + 2 * g + g // 2 + g // 3, lambda g: 3 * g - g // 2),
)


def position():
    ep = lax.axis_index('ep')
    return lax.axis_index('ep2'), ep // 2, ep % 2


def partner(where, k):
    y, x, c = where
    py = (y + k // 4) % 2
    px = (x + (k // 2) % 2) % 2
    pc = (c + k % 2) % 2
    return py * 4 + px * 2 + pc, {'ep2': py, 'ep': px * 2 + pc}


def greet(where):
    barrier = pltpu.get_barrier_semaphore()
    for k in range(1, GROUP):
        pl.semaphore_signal(barrier, inc=1, device_id=partner(where, k)[1], device_id_type=MESH)
    pl.semaphore_wait(barrier, GROUP - 1)


def route_kernel(capacity, ids_ref, gate_ref, qrow_ref, qcol_ref, dl_ref, dr_ref, sel_ref,
                 cbuf, kept_ref, off_ref, start_ref, tot_ref, mat_ref, mat_t, rank_ref, wide_ref, drow_ref,
                 send_sem, recv_sem):
    where = position()
    me = where[0] * 4 + where[1] * 2 + where[2]
    n_tok = ids_ref.shape[1]
    experts = 128
    e_loc = experts // GROUP

    hot = jnp.where(lax.broadcasted_iota(jnp.int32, (experts, n_tok), 0) == ids_ref[...], 1.0, 0.0).astype(BF16)
    cbuf[0] = lax.dot_general(jnp.ones((8, n_tok), BF16), hot, (((1,), (1,)), ((), ())), preferred_element_type=F32)

    greet(where)

    def count_copy(k):
        return pltpu.make_async_remote_copy(
            src_ref=cbuf.at[0], dst_ref=cbuf.at[k], send_sem=send_sem.at[k], recv_sem=recv_sem.at[k],
            device_id=partner(where, k)[1], device_id_type=MESH)

    for k in range(1, GROUP):
        count_copy(k).start()

    blk = 256
    upper = jnp.where(lax.broadcasted_iota(jnp.int32, (blk, blk), 0) < lax.broadcasted_iota(jnp.int32, (blk, blk), 1), 1.0, 0.0).astype(BF16)
    base = jnp.zeros((experts, 1), F32)
    for b in range(n_tok // blk):
        hot_b = hot[:, b * blk:(b + 1) * blk]
        rank_ref[:, b * blk:(b + 1) * blk] = jnp.dot(hot_b, upper, preferred_element_type=F32) + base
        base = base + jnp.sum(hot_b.astype(F32), axis=1, keepdims=True)

    for k in range(1, GROUP):
        count_copy(k).wait_recv()

    run = jnp.zeros((1, experts), F32)
    for s in range(GROUP):
        k = ((where[0] + s // 4) % 2) * 4 + ((where[1] + (s // 2) % 2) % 2) * 2 + (where[2] + s % 2) % 2
        cnt = cbuf[k, 0:1, :]
        off_ref[s:s + 1, :] = run
        kept_ref[s:s + 1, :] = jnp.minimum(jnp.maximum(capacity - run, 0.0), cnt)
        run = run + cnt
    kept = kept_ref[...]
    row_e = lax.broadcasted_iota(jnp.int32, (experts, experts), 0)
    col_e = lax.broadcasted_iota(jnp.int32, (experts, experts), 1)
    same = (row_e // e_loc) == (col_e // e_loc)
    before = jnp.where(same & (row_e < col_e), 1.0, 0.0).astype(BF16)
    block = jnp.where(same, 1.0, 0.0).astype(BF16)
    start = jnp.dot(kept.astype(BF16), before, preferred_element_type=F32)
    total = jnp.dot(kept.astype(BF16), block, preferred_element_type=F32)
    start_ref[...] = start
    tot_ref[...] = total

    last = lax.broadcasted_iota(jnp.int32, (8, experts), 1) % e_loc
    head = start + kept
    tail = total - head
    choice = jnp.zeros((8, experts), F32)
    for plan in PLANS[:-1]:
        caps = plan.caps()
        over = jnp.where(total > caps[3], 1.0, 0.0)
        for g in range(3):
            over = jnp.maximum(over, jnp.where((last == 4 * g + 3) & (head > caps[g]), 1.0, 0.0))
            over = jnp.maximum(over, jnp.where((last == 4 * g + 3) & (tail > caps[2 - g]), 1.0, 0.0))
        choice = choice + jnp.max(over, keepdims=True)
    sel_ref[...] = choice.astype(jnp.int32)

    mat_ref[...] = jnp.zeros_like(mat_ref)
    lane_k = jnp.bitwise_xor(lax.broadcasted_iota(jnp.int32, (1, experts), 1) // e_loc, me).astype(F32)
    my_start = start_ref[pl.ds(me, 1), :]
    my_code = lane_k * SPAN + my_start
    mat_ref[0:1, :] = kept_ref[pl.ds(me, 1), :]
    mat_ref[1:2, :] = my_code + 1.0
    mat_ref[2:3, :] = my_code + (SPAN + 1.0) - tot_ref[pl.ds(me, 1), :]
    for k in range(GROUP):
        s = partner(where, k)[0]
        mat_ref[8 + k:9 + k, :] = kept_ref[pl.ds(s, 1), :]
        mat_ref[16 + k:17 + k, :] = off_ref[pl.ds(s, 1), :]
        mat_ref[24 + k:25 + k, :] = start_ref[pl.ds(s, 1), :]
        mat_ref[32 + k:33 + k, :] = tot_ref[pl.ds(s, 1), :]
    mat_t[...] = jnp.transpose(mat_ref[...])

    wide_ref[...] = jnp.zeros_like(wide_ref)
    hot_f = hot.astype(F32)
    rank = rank_ref[...]
    live = jnp.where(rank < mat_t[:, 0:1], hot_f, 0.0)
    qrow_ref[...] = jnp.broadcast_to(jnp.sum(live * (rank + mat_t[:, 1:2]), axis=0, keepdims=True) - 1.0, qrow_ref.shape)
    wide_ref[0:1, :] = jnp.sum(live * (rank + mat_t[:, 2:3]), axis=0, keepdims=True) - 1.0
    wide_ref[1:2, :] = gate_ref[...]
    qcol_ref[...] = jnp.transpose(wide_ref[...])

    drow_ref[...] = jnp.zeros_like(drow_ref)
    mine = mat_t[pl.ds(pl.multiple_of(me * e_loc, e_loc), e_loc), :]
    pos = lax.broadcasted_iota(jnp.int32, (e_loc, SPAN), 1).astype(F32)
    slot0 = lax.broadcasted_iota(jnp.int32, (e_loc, SPAN), 0).astype(F32) * capacity
    for k in range(GROUP):
        kept_c, off_c, start_c, tot_c = (mine[:, r + k:r + k + 1] for r in (8, 16, 24, 32))

        def slots(p):
            inside = (p >= start_c) & (p < start_c + kept_c)
            return jnp.sum(jnp.where(inside, slot0 + off_c + p - start_c + 1.0, 0.0), axis=0, keepdims=True) - 1.0

        dl_ref[k:k + 1, :] = slots(pos)
        drow_ref[k:k + 1, :] = slots(pos - (SPAN - tot_c))
    dr_ref[...] = jnp.transpose(drow_ref[...])

    for k in range(1, GROUP):
        count_copy(k).wait_send()


def moe_kernel(plan, capacity, x_ref, qrow_ref, qcol_ref, dl_ref, dr_ref, w_in, w_out, y_ref,
               send, recv, rsend, rrecv, bbuf, obuf, got, acc, wi, wo, dlc, drc, tcol, trow, icol,
               s_send, s_recv, r_send, r_recv, wi_sem, wo_sem):
    nc, ns = plan.chunks, plan.slots
    rows = GROUP * ZROWS
    n_tok, d_model = x_ref.shape
    e_loc, _, ff = w_in.shape
    per_e = ff // FTILE
    quad = 4 * capacity
    where = position()

    def w_copies(i, slot):
        e, f = i // per_e, i % per_e
        cols = pl.ds(pl.multiple_of(f * FTILE, FTILE), FTILE)
        return (pltpu.make_async_copy(w_in.at[e, :, cols], wi.at[slot], wi_sem.at[slot]),
                pltpu.make_async_copy(w_out.at[e, cols, :], wo.at[slot], wo_sem.at[slot]))

    for i in range(ns):
        for copy in w_copies(i, i):
            copy.start()

    def out_copy(c, k):
        return pltpu.make_async_remote_copy(
            src_ref=send.at[c, k], dst_ref=recv.at[c, k], send_sem=s_send.at[c, k], recv_sem=s_recv.at[c, k],
            device_id=partner(where, k)[1], device_id_type=MESH)

    def back_copy(c, k):
        return pltpu.make_async_remote_copy(
            src_ref=rsend.at[c, k], dst_ref=rrecv.at[c, k], send_sem=r_send.at[c, k], recv_sem=r_recv.at[c, k],
            device_id=partner(where, k)[1], device_id_type=MESH)

    def targets(shape, dim):
        i = lax.broadcasted_iota(jnp.int32, shape, dim)
        k = jnp.zeros(shape, jnp.int32)
        for m in range(1, GROUP):
            k = k + jnp.where(i >= m * ZROWS, 1, 0)
        return (i + k * (SPAN - ZROWS)).astype(F32)

    tcol[...] = targets(tcol.shape, 0)
    trow[...] = targets(trow.shape, 1) + float(SPAN - nc * ZROWS)
    icol[...] = lax.broadcasted_iota(jnp.int32, icol.shape, 0).astype(F32)

    greet(where)

    def hot_of(a, b):
        return jnp.where(a == b, 1.0, 0.0).astype(BF16)

    @pl.loop(0, nc)
    def _(c):
        want = tcol[:, 0:1] + (c * ZROWS).astype(F32)
        packed = jnp.dot(hot_of(want, qrow_ref[0:1, :]), x_ref[...], preferred_element_type=F32).astype(BF16)
        send[c] = packed.reshape(GROUP, ZROWS, d_model)
        recv[c, 0] = send[c, 0]
        for k in range(GROUP - 1, 0, -1):
            out_copy(c, k).start()

    for c in range(nc):
        for k in range(GROUP):
            dlc[c, 0:1, k * ZROWS:(k + 1) * ZROWS] = dl_ref[k:k + 1, c * ZROWS:(c + 1) * ZROWS]
            first = SPAN - nc * ZROWS + c * ZROWS
            drc[c, k * ZROWS:(k + 1) * ZROWS, :] = dr_ref[first:first + ZROWS, k:k + 1]

    @pl.loop(0, 4)
    def _(g):
        @pl.loop(plan.need_lo(g), plan.need(g))
        def _(c):
            for k in range(1, GROUP):
                out_copy(c, k).wait_recv()

        acc[...] = jnp.zeros_like(acc)

        @pl.loop(0, plan.need(g))
        def _(c):
            slot_row = dlc[c, 0:1, :] - (g * quad).astype(F32)
            acc[...] += jnp.dot(hot_of(icol[:, 0:1], slot_row), recv[c].reshape(rows, d_model), preferred_element_type=F32)

        bbuf[...] = acc[...].astype(BF16)

        @pl.loop(0, 4)
        def _(j):
            e = g * 4 + j
            at = pl.ds(pl.multiple_of(j * capacity, capacity), capacity)
            total = None
            for f in range(per_e):
                i = e * per_e + f
                slot = i % ns
                for copy in w_copies(i, slot):
                    copy.wait()
                v = jnp.dot(bbuf[at, :], wi[slot], preferred_element_type=F32)
                h = 0.5 * v * (1.0 + jnp.tanh(0.7978845608028654 * (v + 0.044715 * (v * v * v))))
                part = jnp.dot(h.astype(BF16), wo[slot], preferred_element_type=F32)
                total = part if total is None else total + part

                @pl.when(i + ns < e_loc * per_e)
                def _():
                    for copy in w_copies(i + ns, slot):
                        copy.start()
            obuf[g, at, :] = total.astype(BF16)

        @pl.loop(plan.free_lo(g), plan.free(g))
        def _(c):
            acc[0:rows, :] = jnp.zeros((rows, d_model), F32)

            @pl.loop(0, g + 1)
            def _(m):
                slot_row = lax.broadcasted_iota(jnp.int32, (1, quad), 1).astype(F32) + (m * quad).astype(F32)
                acc[0:rows, :] += jnp.dot(hot_of(drc[c], slot_row), obuf[m], preferred_element_type=F32)

            rsend[c] = acc[0:rows, :].astype(BF16).reshape(GROUP, ZROWS, d_model)
            rrecv[c, 0] = rsend[c, 0]
            for k in range(GROUP - 1, 0, -1):
                back_copy(c, k).start()

    tt = 256
    got[...] = jnp.zeros_like(got)

    @pl.loop(0, nc)
    def _(c):
        for k in range(1, GROUP):
            back_copy(c, k).wait_recv()
        want = trow[0:1, :] + (c * ZROWS).astype(F32)

        @pl.loop(0, n_tok // tt)
        def _(t):
            at = pl.ds(pl.multiple_of(t * tt, tt), tt)
            got[at, :] += jnp.dot(hot_of(qcol_ref[at, 0:1], want), rrecv[c].reshape(rows, d_model),
                                  preferred_element_type=F32).astype(BF16)

    @pl.loop(0, n_tok // tt)
    def _(t):
        at = pl.ds(pl.multiple_of(t * tt, tt), tt)
        y_ref[at, :] = (x_ref[at, :].astype(F32) + qcol_ref[at, 1:2] * got[at, :].astype(F32)).astype(BF16)

    @pl.loop(0, nc)
    def _(c):
        for k in range(1, GROUP):
            out_copy(c, k).wait_send()
            back_copy(c, k).wait_send()


def solution(mesh):
    dev_axes = ('ep2', 'ep')

    def local_step(x_loc, ids_loc, gate_loc, w_a, w_b):
        n_tok, d_model = x_loc.shape
        e_loc, _, ff = w_a.shape
        experts = e_loc * GROUP
        capacity = 8 * ((5 * GROUP * n_tok) // (32 * experts))
        vmem = pl.BlockSpec(memory_space=pltpu.VMEM)
        hbm = pl.BlockSpec(memory_space=pl.ANY)

        qrow, qcol, dl, dr, sel = pl.pallas_call(
            functools.partial(route_kernel, capacity),
            out_shape=(jax.ShapeDtypeStruct((8, n_tok), F32), jax.ShapeDtypeStruct((n_tok, 128), F32),
                       jax.ShapeDtypeStruct((8, SPAN), F32), jax.ShapeDtypeStruct((SPAN, 128), F32),
                       jax.ShapeDtypeStruct((8, experts), jnp.int32)),
            in_specs=[vmem] * 2, out_specs=(vmem,) * 5,
            scratch_shapes=[
                pltpu.VMEM((GROUP, 8, experts), F32),
                pltpu.VMEM((8, experts), F32), pltpu.VMEM((8, experts), F32),
                pltpu.VMEM((8, experts), F32), pltpu.VMEM((8, experts), F32),
                pltpu.VMEM((128, experts), F32), pltpu.VMEM((experts, 128), F32),
                pltpu.VMEM((experts, n_tok), F32), pltpu.VMEM((128, n_tok), F32), pltpu.VMEM((128, SPAN), F32),
                pltpu.SemaphoreType.DMA((GROUP,)), pltpu.SemaphoreType.DMA((GROUP,)),
            ],
            compiler_params=pltpu.CompilerParams(collective_id=0, has_side_effects=True),
            name='route',
        )(ids_loc.reshape(1, n_tok), gate_loc.reshape(1, n_tok))

        def variant(number):
            plan = PLANS[number]
            nc, ns = plan.chunks, plan.slots
            rows = GROUP * ZROWS
            block = (nc, GROUP, ZROWS, d_model)

            def call(x_loc, qrow, qcol, dl, dr, w_a, w_b):
                return pl.pallas_call(
                    functools.partial(moe_kernel, plan, capacity),
                    out_shape=jax.ShapeDtypeStruct((n_tok, d_model), BF16),
                    in_specs=[vmem] * 5 + [hbm] * 2, out_specs=vmem,
                    scratch_shapes=[
                        pltpu.VMEM(block, BF16), pltpu.VMEM(block, BF16), pltpu.VMEM(block, BF16), pltpu.VMEM(block, BF16),
                        pltpu.VMEM((4 * capacity, d_model), BF16), pltpu.VMEM((4, 4 * capacity, d_model), BF16),
                        pltpu.VMEM((n_tok, d_model), BF16), pltpu.VMEM((4 * capacity, d_model), F32),
                        pltpu.VMEM((ns, d_model, FTILE), BF16), pltpu.VMEM((ns, FTILE, d_model), BF16),
                        pltpu.VMEM((nc, 8, rows), F32), pltpu.VMEM((nc, rows, 1), F32),
                        pltpu.VMEM((rows, 128), F32), pltpu.VMEM((8, rows), F32), pltpu.VMEM((4 * capacity, 128), F32),
                        pltpu.SemaphoreType.DMA((nc, GROUP)), pltpu.SemaphoreType.DMA((nc, GROUP)),
                        pltpu.SemaphoreType.DMA((nc, GROUP)), pltpu.SemaphoreType.DMA((nc, GROUP)),
                        pltpu.SemaphoreType.DMA((ns,)), pltpu.SemaphoreType.DMA((ns,)),
                    ],
                    compiler_params=pltpu.CompilerParams(
                        collective_id=1 + number, has_side_effects=True, vmem_limit_bytes=66_000_000),
                    name='moe_' + str(nc),
                )(x_loc, qrow, qcol, dl, dr, w_a, w_b)

            return call

        return lax.switch(sel[0, 0], [variant(i) for i in range(len(PLANS))], x_loc, qrow, qcol, dl, dr, w_a, w_b)

    tok_spec = P(('dp', 'ep2', 'ep'), None)
    w_spec = P(dev_axes, None, None)
    return jax.shard_map(local_step, mesh=mesh, in_specs=(tok_spec, tok_spec, tok_spec, w_spec, w_spec), out_specs=tok_spec, check_vma=False)
```

```python
import functools

import jax
import jax.numpy as jnp
from jax import lax
from jax.experimental import pallas as pl
from jax.experimental.pallas import tpu as pltpu
from jax.sharding import PartitionSpec as P

MESH = pl.DeviceIdType.MESH
F32 = jnp.float32
BF16 = jnp.bfloat16
GROUP = 8
EXPERTS = 128
E_LOC = EXPERTS // GROUP
SPAN = 640
Z = 48
ROWS = GROUP * Z
FTILE = 1536
TTILE = 256


def pick(values, i):
    out = values[0]
    for m in range(1, len(values)):
        out = out + (values[m] - values[m - 1]) * ((i + 16 - m) // 16)
    return out


class Plan:
    def __init__(self, lo, hi, slots):
        self.lo, self.hi, self.slots = lo, hi, slots
        self.chunks = hi[-1]
        self.hi_before = (0,) + hi[:-1]
        self.lo_next = lo[1:] + (self.chunks,)
        span = range(self.chunks)
        self.first = tuple(min(m for m in range(4) if hi[m] > c) for c in span)
        self.after = tuple(max(m for m in range(4) if lo[m] <= c) + 1 for c in span)


FAST = Plan((0, 1, 2, 4), (3, 4, 6, 7), 5)
SAFE = Plan((0, 0, 0, 0), (3, 6, 8, 11), 3)


def position():
    ep = lax.axis_index('ep')
    return lax.axis_index('ep2'), ep // 2, ep % 2


def partner(where, k):
    y, x, c = where
    py = (y + k // 4) % 2
    px = (x + (k // 2) % 2) % 2
    pc = (c + k % 2) % 2
    return py * 4 + px * 2 + pc, {'ep2': py, 'ep': px * 2 + pc}


def iota(shape, dim):
    return lax.broadcasted_iota(jnp.int32, shape, dim)


def hot(mask):
    return jnp.where(mask, 1.0, 0.0).astype(BF16)


def dot(a, b):
    return jnp.dot(a, b, preferred_element_type=F32)


def moe_kernel(plan, capacity, ids_ref, x_hbm, w_in, w_out, got, flag_ref,
               xv, send, recv, rsend, rrecv, bbuf, obuf, acc, wi, wo, xbuf, cbuf, qrow, qcol, dlc, drc,
               x_sem, n_send, n_recv, s_send, s_recv, r_send, r_recv, wi_sem, wo_sem):
    nc, ns = plan.chunks, plan.slots
    n_tok, d_model = xv.shape
    per_e = w_in.shape[2] // FTILE
    quad = 4 * capacity
    where = position()
    me = partner(where, 0)[0]

    def w_copies(i, slot):
        e, f = i // per_e, i % per_e
        cols = pl.ds(pl.multiple_of(f * FTILE, FTILE), FTILE)
        return (pltpu.make_async_copy(w_in.at[e, :, cols], wi.at[slot], wi_sem.at[slot]),
                pltpu.make_async_copy(w_out.at[e, cols, :], wo.at[slot], wo_sem.at[slot]))

    def remote(src, dst, sent, received, k):
        return pltpu.make_async_remote_copy(src_ref=src, dst_ref=dst, send_sem=sent, recv_sem=received,
                                            device_id=partner(where, k)[1], device_id_type=MESH)

    def count_copy(k):
        return remote(xbuf.at[k], cbuf.at[k], n_send.at[k], n_recv.at[k], k)

    def out_copy(c, k):
        return remote(send.at[c, k], recv.at[c, k], s_send.at[c, k], s_recv.at[c, k], k)

    def back_copy(c, k):
        return remote(rsend.at[c, k], rrecv.at[c, k], r_send.at[c, k], r_recv.at[c, k], k)

    barrier = pltpu.get_barrier_semaphore()
    for k in range(1, GROUP):
        pl.semaphore_signal(barrier, inc=1, device_id=partner(where, k)[1], device_id_type=MESH)
    x_copy = pltpu.make_async_copy(x_hbm, xv, x_sem)
    x_copy.start()
    for i in range(ns):
        for copy in w_copies(i, i):
            copy.start()

    row, col = iota((EXPERTS, EXPERTS), 0), iota((EXPERTS, EXPERTS), 1)
    same = (row // E_LOC) == (col // E_LOC)
    in_row, in_col = (row % E_LOC) // 4, (col % E_LOC) // 4
    inner = hot(same & (in_row == in_col) & (col < row))
    sums = [hot(same & (in_col == g)) for g in range(4)]

    def starts(counts):
        counts = counts.astype(BF16)
        base = jnp.zeros((EXPERTS, EXPERTS), F32)
        mine, over = base, base
        for g in range(4):
            if g:
                base = jnp.maximum(base, float(plan.lo[g] * Z))
            mine = jnp.where(in_row == g, base, mine)
            base = base + dot(sums[g], counts)
            over = jnp.maximum(over, base - float(plan.hi[g] * Z))
        return mine + dot(inner, counts), over

    chosen = hot(iota((EXPERTS, n_tok), 0) == ids_ref[...])
    counts = dot(chosen, jnp.ones((n_tok, 128), BF16))
    start, over = starts(counts)
    to_k = jnp.bitwise_xor(row // E_LOC, me).astype(F32)
    code0 = to_k * float(SPAN) + start

    upper = hot((iota((TTILE, TTILE + 128), 0) < iota((TTILE, TTILE + 128), 1)) | (iota((TTILE, TTILE + 128), 1) >= TTILE))
    base = code0
    for b in range(n_tok // TTILE):
        part = chosen[:, b * TTILE:(b + 1) * TTILE]
        rank = dot(part, upper)
        full = jnp.concatenate([rank[:, i * 128:(i + 1) * 128] + base for i in range(TTILE // 128)], axis=1)
        code = jnp.sum(part.astype(F32) * full, axis=0, keepdims=True)
        qrow[:, b * TTILE:(b + 1) * TTILE] = jnp.broadcast_to(code, (8, TTILE))
        base = base + rank[:, TTILE:]

    worst = jnp.broadcast_to(jnp.max(over, keepdims=True), (8, 128))
    acc[0:EXPERTS, 0:128] = counts
    for k in range(GROUP):
        at = pl.ds(pl.multiple_of(partner(where, k)[0] * E_LOC, E_LOC), E_LOC)
        xbuf[k, 0:E_LOC, :] = acc[at, 0:128]
        xbuf[k, E_LOC:E_LOC + 8, :] = worst
    cbuf[0] = xbuf[0]

    def targets(shape, dim):
        i = iota(shape, dim)
        c = jnp.where(i >= ROWS, 1, 0)
        i = i - c * ROWS
        k = jnp.zeros(shape, jnp.int32)
        for m in range(1, GROUP):
            k = k + jnp.where(i >= m * Z, 1, 0)
        return (i + k * (SPAN - Z) + c * Z).astype(F32)

    tcol = targets((ROWS, 1), 0)
    trow = targets((1, 2 * ROWS), 1)

    pl.semaphore_wait(barrier, GROUP - 1)
    for k in range(1, GROUP):
        count_copy(k).start()
    x_copy.wait()

    @pl.loop(0, nc)
    def _(c):
        mask = (tcol + (c * Z).astype(F32)) == qrow[0:1, :]
        send[c] = dot(hot(mask), xv[...]).astype(BF16).reshape(GROUP, Z, d_model)
        for k in range(GROUP - 1, 0, -1):
            out_copy(c, k).start()
        recv[c, 0] = send[c, 0]

    for b in range(n_tok // TTILE):
        piece = jnp.broadcast_to(qrow[0:1, b * TTILE:(b + 1) * TTILE], (128, TTILE))
        qcol[b * TTILE:(b + 1) * TTILE, :] = jnp.transpose(piece)
    for k in range(1, GROUP):
        count_copy(k).wait_recv()
    flag_ref[...] = jnp.where(jnp.max(cbuf[:, E_LOC:E_LOC + 8, :], axis=0) > 0.0, 1, 0)
    got_counts = cbuf[:, 0:E_LOC, :].reshape(EXPERTS, 128)
    start, _ = starts(got_counts)
    earlier = hot(((row % E_LOC) == (col % E_LOC)) & (jnp.bitwise_xor(col // E_LOC, me) < jnp.bitwise_xor(row // E_LOC, me)))
    ahead = dot(earlier, got_counts.astype(BF16))
    first = ((row // E_LOC) * SPAN).astype(F32) + start
    kept = jnp.minimum(got_counts, jnp.maximum(capacity - ahead, 0.0))
    last = first + kept
    shift = ((row % E_LOC) * capacity + 1).astype(F32) + ahead - first
    first, last, shift = first[:, 0:1], last[:, 0:1], shift[:, 0:1]
    for c in range(nc):
        at = trow[:, 0:ROWS] + float(c * Z)
        slot = jnp.sum(jnp.where((at >= first) & (at < last), at + shift, 0.0), axis=0, keepdims=True) - 1.0
        dlc[c] = jnp.broadcast_to(slot, (8, ROWS))
        drc[c] = jnp.transpose(jnp.broadcast_to(slot, (128, ROWS)))

    slot_col = iota((quad, 1), 0).astype(F32)
    slot_row = iota((1, quad), 1).astype(F32)

    @pl.loop(0, 4)
    def _(g):
        @pl.loop(pick(plan.hi_before, g), pick(plan.hi, g))
        def _(c):
            for k in range(1, GROUP):
                out_copy(c, k).wait_recv()

        acc[...] = jnp.zeros_like(acc)

        @pl.loop(pick(plan.lo, g), pick(plan.hi, g))
        def _(c):
            mask = (slot_col + (g * quad).astype(F32)) == dlc[c, 0:1, :]
            acc[...] += dot(hot(mask), recv[c].reshape(ROWS, d_model))

        bbuf[...] = acc[...].astype(BF16)

        @pl.loop(0, 4)
        def _(j):
            at = pl.ds(pl.multiple_of(j * capacity, capacity), capacity)
            first_i = (g * 4 + j) * per_e
            for f in range(per_e):
                for copy in w_copies(first_i + f, (first_i + f) % ns):
                    copy.wait()
            total = None
            for f in range(per_e):
                slot = (first_i + f) % ns
                for h in range(2):
                    cols = slice(h * FTILE // 2, (h + 1) * FTILE // 2)
                    v = dot(bbuf[at, :], wi[slot, :, cols])
                    u = v * (0.7978845608028654 + (0.7978845608028654 * 0.044715) * (v * v))
                    half = 0.5 * v
                    part = dot((half + half * jnp.tanh(u)).astype(BF16), wo[slot, cols, :])
                    total = part if total is None else total + part
            obuf[g, at, :] = total.astype(BF16)
            for f in range(per_e):
                @pl.when(first_i + f + ns < E_LOC * per_e)
                def _():
                    for copy in w_copies(first_i + f + ns, (first_i + f) % ns):
                        copy.start()

        @pl.loop(pick(plan.lo, g), pick(plan.lo_next, g))
        def _(c):
            acc[0:ROWS, :] = jnp.zeros((ROWS, d_model), F32)

            @pl.loop(pick(plan.first, c), pick(plan.after, c))
            def _(m):
                mask = drc[c, :, 0:1] == (slot_row + (m * quad).astype(F32))
                acc[0:ROWS, :] += dot(hot(mask), obuf[m])

            rsend[c] = acc[0:ROWS, :].astype(BF16).reshape(GROUP, Z, d_model)
            for k in range(GROUP - 1, 0, -1):
                back_copy(c, k).start()
            rrecv[c, 0] = rsend[c, 0]

    def combine(c, count, fresh):
        want = trow[:, 0:count * ROWS] + (c * Z if isinstance(c, int) else (c * Z).astype(F32))
        for m in range(count):
            for k in range(1, GROUP):
                back_copy(c + m, k).wait_recv()

        @pl.loop(0, n_tok // TTILE)
        def _(t):
            at = pl.ds(pl.multiple_of(t * TTILE, TTILE), TTILE)
            rows = rrecv[pl.ds(c, count)].reshape(count * ROWS, d_model)
            new = dot(hot(qcol[at, 0:1] == want), rows).astype(BF16)
            got[at, :] = new if fresh else got[at, :] + new

    combine(0, 2, True)

    @pl.loop(1, nc // 2)
    def _(p):
        combine(2 * p, 2, False)

    if nc % 2:
        combine(nc - 1, 1, False)

    for k in range(1, GROUP):
        count_copy(k).wait_send()

    @pl.loop(0, nc)
    def _(c):
        for k in range(1, GROUP):
            out_copy(c, k).wait_send()
            back_copy(c, k).wait_send()


def solution(mesh):
    dev_axes = ('ep2', 'ep')

    def local_step(x_loc, ids_loc, gate_loc, w_a, w_b):
        n_tok, d_model = x_loc.shape
        capacity = 8 * ((5 * GROUP * n_tok) // (32 * EXPERTS))
        vmem = pl.BlockSpec(memory_space=pltpu.VMEM)
        hbm = pl.BlockSpec(memory_space=pl.ANY)
        dma = pltpu.SemaphoreType.DMA
        args = (ids_loc.reshape(1, n_tok), x_loc, w_a, w_b)

        def moe(plan, number):
            nc, ns = plan.chunks, plan.slots
            block = pltpu.VMEM((nc, GROUP, Z, d_model), BF16)
            return pl.pallas_call(
                functools.partial(moe_kernel, plan, capacity),
                out_shape=(jax.ShapeDtypeStruct((n_tok, d_model), BF16), jax.ShapeDtypeStruct((8, 128), jnp.int32)),
                in_specs=[vmem] + [hbm] * 3, out_specs=(vmem, vmem),
                scratch_shapes=[
                    pltpu.VMEM((n_tok, d_model), BF16), block, block, block, block,
                    pltpu.VMEM((4 * capacity, d_model), BF16), pltpu.VMEM((4, 4 * capacity, d_model), BF16),
                    pltpu.VMEM((4 * capacity, d_model), F32),
                    pltpu.VMEM((ns, d_model, FTILE), BF16), pltpu.VMEM((ns, FTILE, d_model), BF16),
                    pltpu.VMEM((GROUP, E_LOC + 8, 128), F32), pltpu.VMEM((GROUP, E_LOC + 8, 128), F32),
                    pltpu.VMEM((8, n_tok), F32), pltpu.VMEM((n_tok, 128), F32),
                    pltpu.VMEM((nc, 8, ROWS), F32), pltpu.VMEM((nc, ROWS, 128), F32),
                    dma(()), dma((GROUP,)), dma((GROUP,)),
                    dma((nc, GROUP)), dma((nc, GROUP)), dma((nc, GROUP)), dma((nc, GROUP)), dma((ns,)), dma((ns,)),
                ],
                compiler_params=pltpu.CompilerParams(
                    collective_id=number, has_side_effects=True, vmem_limit_bytes=66_000_000),
                name='moe_' + str(nc),
            )(*args)

        got, flag = moe(FAST, 0)
        got = lax.cond(flag[0, 0] > 0, lambda: moe(SAFE, 1)[0], lambda: got)
        return (x_loc.astype(F32) + gate_loc * got.astype(F32)).astype(BF16)

    tok_spec = P(('dp', 'ep2', 'ep'), None)
    w_spec = P(dev_axes, None, None)
    return jax.shard_map(local_step, mesh=mesh, in_specs=(tok_spec, tok_spec, tok_spec, w_spec, w_spec), out_specs=tok_spec, check_vma=False)
```

```python
import functools

import jax
import jax.numpy as jnp
from jax import lax
from jax.experimental import pallas as pl
from jax.experimental.pallas import tpu as pltpu
from jax.sharding import PartitionSpec as P

MESH = pl.DeviceIdType.MESH
F32 = jnp.float32
BF16 = jnp.bfloat16
GROUP = 8
EXPERTS = 128
E_LOC = EXPERTS // GROUP
SPAN = 512
Z = 32
ROWS = GROUP * Z
PER = 2
SETS = E_LOC // PER
FTILE = 1536
TTILE = 256


def pick(values, i):
    out = values[0]
    for m in range(1, len(values)):
        out = out + (values[m] - values[m - 1]) * ((i + 16 - m) // 16)
    return out


class Plan:
    def __init__(self, lo, hi, slots, batches):
        self.lo, self.hi, self.slots = lo, hi, slots
        self.chunks = hi[-1]
        self.batches = batches
        assert sum(batches) == self.chunks
        self.hi_before = (0,) + hi[:-1]
        self.lo_next = lo[1:] + (self.chunks,)
        self.pairs = tuple((h - l + 1) // 2 for l, h in zip(lo, hi))
        first = [min(m for m in range(SETS) if hi[m] > c) for c in range(self.chunks)]
        after = [max(m for m in range(SETS) if lo[m] <= c) + 1 for c in range(self.chunks)]
        self.wide = max(b - a for a, b in zip(first, after))
        self.first = tuple(min(m, SETS - self.wide) for m in first)
        assert all(h >= 2 * p for h, p in zip(hi, self.pairs))


FAST = Plan((0, 1, 2, 3, 4, 6, 7, 9), (2, 4, 6, 7, 8, 9, 10, 11), 5, (4, 4, 2, 1))
SAFE = Plan((0,) * 8, (2, 4, 6, 8, 10, 12, 14, 16), 3, (4, 4, 4, 4))


def position():
    ep = lax.axis_index('ep')
    return lax.axis_index('ep2'), ep // 2, ep % 2


def partner(where, k):
    y, x, c = where
    py = (y + k // 4) % 2
    px = (x + (k // 2) % 2) % 2
    pc = (c + k % 2) % 2
    return py * 4 + px * 2 + pc, {'ep2': py, 'ep': px * 2 + pc}


def iota(shape, dim):
    return lax.broadcasted_iota(jnp.int32, shape, dim)


def hot(mask):
    return jnp.where(mask, 1.0, 0.0).astype(BF16)


def dot(a, b):
    return jnp.dot(a, b, preferred_element_type=F32)


def moe_kernel(plan, capacity, ids_ref, x_hbm, w_in, w_out, got, flag_ref,
               xv, send, recv, rrecv, bbuf, obuf, acc, wi, wo, xbuf, cbuf, qrow, qcol, dlc, drc,
               x_sem, n_send, n_recv, s_send, s_recv, r_send, r_recv, wi_sem, wo_sem):
    nc, ns = plan.chunks, plan.slots
    n_tok, d_model = xv.shape
    per_e = w_in.shape[2] // FTILE
    slots = PER * capacity
    where = position()
    me = partner(where, 0)[0]

    def w_copies(i, slot):
        e, f = i // per_e, i % per_e
        cols = pl.ds(pl.multiple_of(f * FTILE, FTILE), FTILE)
        return (pltpu.make_async_copy(w_in.at[e, :, cols], wi.at[slot], wi_sem.at[slot]),
                pltpu.make_async_copy(w_out.at[e, cols, :], wo.at[slot], wo_sem.at[slot]))

    def remote(src, dst, sent, received, k):
        return pltpu.make_async_remote_copy(src_ref=src, dst_ref=dst, send_sem=sent, recv_sem=received,
                                            device_id=partner(where, k)[1], device_id_type=MESH)

    def count_copy(k):
        return remote(xbuf.at[k], cbuf.at[k], n_send.at[k], n_recv.at[k], k)

    def out_copy(c, k):
        return remote(send.at[c, k], recv.at[c, k], s_send.at[c, k], s_recv.at[c, k], k)

    def back_copy(c, k):
        return remote(send.at[c, k], rrecv.at[c, k], r_send.at[c, k], r_recv.at[c, k], k)

    barrier = pltpu.get_barrier_semaphore()
    for k in range(1, GROUP):
        pl.semaphore_signal(barrier, inc=1, device_id=partner(where, k)[1], device_id_type=MESH)
    x_copy = pltpu.make_async_copy(x_hbm, xv, x_sem)
    x_copy.start()

    obuf[...] = jnp.zeros_like(obuf)

    row, col = iota((EXPERTS, EXPERTS), 0), iota((EXPERTS, EXPERTS), 1)
    same = (row // E_LOC) == (col // E_LOC)
    in_row, in_col = (row % E_LOC) // PER, (col % E_LOC) // PER
    inner = hot(same & (in_row == in_col) & (col < row))
    sums = [hot(same & (in_col == g)) for g in range(SETS)]

    def starts(counts):
        counts = counts.astype(BF16)
        base = jnp.zeros((EXPERTS, EXPERTS), F32)
        mine, over = base, base
        for g in range(SETS):
            if g:
                base = jnp.maximum(base, float(plan.lo[g] * Z))
            mine = jnp.where(in_row == g, base, mine)
            base = base + dot(sums[g], counts)
            over = jnp.maximum(over, base - float(plan.hi[g] * Z))
        return mine + dot(inner, counts), over

    chosen = hot(iota((EXPERTS, n_tok), 0) == ids_ref[...])
    counts = dot(chosen, jnp.ones((n_tok, 128), BF16))
    start, over = starts(counts)
    to_k = jnp.bitwise_xor(row // E_LOC, me).astype(F32)
    code0 = to_k * float(SPAN) + start

    upper = hot((iota((TTILE, TTILE + 128), 0) < iota((TTILE, TTILE + 128), 1)) | (iota((TTILE, TTILE + 128), 1) >= TTILE))
    base = code0
    for b in range(n_tok // TTILE):
        part = chosen[:, b * TTILE:(b + 1) * TTILE]
        rank = dot(part, upper)
        full = jnp.concatenate([rank[:, i * 128:(i + 1) * 128] + base for i in range(TTILE // 128)], axis=1)
        code = jnp.sum(part.astype(F32) * full, axis=0, keepdims=True)
        qrow[:, b * TTILE:(b + 1) * TTILE] = jnp.broadcast_to(code, (8, TTILE))
        base = base + rank[:, TTILE:]

    worst = jnp.broadcast_to(jnp.max(over, keepdims=True), (8, 128))
    acc[0:EXPERTS, 0:128] = counts
    for k in range(GROUP):
        at = pl.ds(pl.multiple_of(partner(where, k)[0] * E_LOC, E_LOC), E_LOC)
        xbuf[k, 0:E_LOC, :] = acc[at, 0:128]
        xbuf[k, E_LOC:E_LOC + 8, :] = worst
    cbuf[0] = xbuf[0]

    def targets(shape, dim):
        i = iota(shape, dim)
        k = jnp.zeros(shape, jnp.int32)
        c = k
        for m in range(1, -(-shape[dim] // ROWS)):
            c = c + jnp.where(i >= m * ROWS, 1, 0)
        i = i - c * ROWS
        for m in range(1, GROUP):
            k = k + jnp.where(i >= m * Z, 1, 0)
        return (i + k * (SPAN - Z) + c * Z).astype(F32)

    tcol = targets((ROWS, 1), 0)
    trow = targets((1, 4 * ROWS), 1)

    pl.semaphore_wait(barrier, GROUP - 1)
    for k in range(1, GROUP):
        count_copy(k).start()
    x_copy.wait()
    for i in range(ns):
        for copy in w_copies(i, i):
            copy.start()

    @pl.loop(0, nc)
    def _(c):
        mask = (tcol + (c * Z).astype(F32)) == qrow[0:1, :]
        send[c] = dot(hot(mask), xv[...]).astype(BF16).reshape(GROUP, Z, d_model)
        for k in range(GROUP - 1, 0, -1):
            out_copy(c, k).start()
        recv[c, 0] = send[c, 0]

    for b in range(n_tok // TTILE):
        piece = jnp.broadcast_to(qrow[0:1, b * TTILE:(b + 1) * TTILE], (128, TTILE))
        qcol[b * TTILE:(b + 1) * TTILE, :] = jnp.transpose(piece)
    for k in range(1, GROUP):
        count_copy(k).wait_recv()
    flag_ref[0, 0] = jnp.max(cbuf[:, E_LOC:E_LOC + 8, :])
    got_counts = cbuf[:, 0:E_LOC, :].reshape(EXPERTS, 128)
    start, _ = starts(got_counts)
    earlier = hot(((row % E_LOC) == (col % E_LOC)) & (jnp.bitwise_xor(col // E_LOC, me) < jnp.bitwise_xor(row // E_LOC, me)))
    ahead = dot(earlier, got_counts.astype(BF16))
    first = ((row // E_LOC) * SPAN).astype(F32) + start
    kept = jnp.minimum(got_counts, jnp.maximum(capacity - ahead, 0.0))
    last = first + kept
    shift = ((row % E_LOC) * capacity + 1).astype(F32) + ahead - first
    first, last, shift = first[:, 0:1], last[:, 0:1], shift[:, 0:1]
    for c in range(nc):
        at = trow[:, 0:ROWS] + float(c * Z)
        slot = jnp.sum(jnp.where((at >= first) & (at < last), at + shift, 0.0), axis=0, keepdims=True) - 1.0
        dlc[c] = jnp.broadcast_to(slot, (8, ROWS))
        drc[c] = jnp.transpose(jnp.broadcast_to(slot, (128, ROWS)))

    slot_col = iota((slots, 1), 0).astype(F32)
    slot_row = iota((1, plan.wide * slots), 1).astype(F32)

    @pl.loop(0, SETS)
    def _(g):
        @pl.loop(pick(plan.hi_before, g), pick(plan.hi, g))
        def _(c):
            for k in range(1, GROUP):
                out_copy(c, k).wait_recv()

        acc[...] = jnp.zeros_like(acc)

        @pl.loop(0, pick(plan.pairs, g))
        def _(p):
            c = pick(plan.hi, g) - 2 * p - 2
            slot = jnp.concatenate([dlc[c, 0:1, :], dlc[c + 1, 0:1, :]], axis=1)
            mask = (slot_col + (g * slots).astype(F32)) == slot
            acc[...] += dot(hot(mask), recv[pl.ds(c, 2)].reshape(2 * ROWS, d_model))

        bbuf[...] = acc[...].astype(BF16)

        @pl.loop(0, PER)
        def _(j):
            at = pl.ds(pl.multiple_of(j * capacity, capacity), capacity)
            first_i = (g * PER + j) * per_e
            total = None
            for f in range(per_e):
                i = first_i + f
                slot = i % ns
                for copy in w_copies(i, slot):
                    copy.wait()
                v = dot(bbuf[at, :], wi[slot])
                u = v * (0.7978845608028654 + (0.7978845608028654 * 0.044715) * (v * v))
                half = 0.5 * v
                part = dot((half + half * jnp.tanh(u)).astype(BF16), wo[slot])
                total = part if total is None else total + part

                @pl.when(i + ns < E_LOC * per_e)
                def _():
                    for copy in w_copies(i + ns, slot):
                        copy.start()
            obuf[g, at, :] = total.astype(BF16)

        @pl.loop(pick(plan.lo, g), pick(plan.lo_next, g))
        def _(c):
            m = pick(plan.first, c)
            mask = drc[c, :, 0:1] == (slot_row + (m * slots).astype(F32))
            packed = dot(hot(mask), obuf[pl.ds(m, plan.wide)].reshape(plan.wide * slots, d_model)).astype(BF16)
            for k in range(1, GROUP):
                out_copy(c, k).wait_send()
            send[c] = packed.reshape(GROUP, Z, d_model)
            for k in range(GROUP - 1, 0, -1):
                back_copy(c, k).start()
            rrecv[c, 0] = send[c, 0]

    def combine(c, count, fresh):
        want = trow[:, 0:count * ROWS] + float(c * Z)
        for m in range(count):
            for k in range(1, GROUP):
                back_copy(c + m, k).wait_recv()

        @pl.loop(0, n_tok // TTILE)
        def _(t):
            at = pl.ds(pl.multiple_of(t * TTILE, TTILE), TTILE)
            rows = rrecv[c:c + count].reshape(count * ROWS, d_model)
            new = dot(hot(qcol[at, 0:1] == want), rows).astype(BF16)
            got[at, :] = new if fresh else got[at, :] + new

    c = 0
    for count in plan.batches:
        combine(c, count, c == 0)
        c += count

    for k in range(1, GROUP):
        count_copy(k).wait_send()

    @pl.loop(0, nc)
    def _(c):
        for k in range(1, GROUP):
            back_copy(c, k).wait_send()


def solution(mesh):
    dev_axes = ('ep2', 'ep')

    def local_step(x_loc, ids_loc, gate_loc, w_a, w_b):
        n_tok, d_model = x_loc.shape
        capacity = 8 * ((5 * GROUP * n_tok) // (32 * EXPERTS))
        vmem = pl.BlockSpec(memory_space=pltpu.VMEM)
        hbm = pl.BlockSpec(memory_space=pl.ANY)
        dma = pltpu.SemaphoreType.DMA
        args = (ids_loc.reshape(1, n_tok), x_loc, w_a, w_b)

        def moe(plan, number):
            nc, ns = plan.chunks, plan.slots
            block = pltpu.VMEM((nc, GROUP, Z, d_model), BF16)
            return pl.pallas_call(
                functools.partial(moe_kernel, plan, capacity),
                out_shape=(jax.ShapeDtypeStruct((n_tok, d_model), BF16), jax.ShapeDtypeStruct((1, 1), F32)),
                in_specs=[vmem] + [hbm] * 3, out_specs=(vmem, pl.BlockSpec(memory_space=pltpu.SMEM)),
                scratch_shapes=[
                    pltpu.VMEM((n_tok, d_model), BF16), block, block, block,
                    pltpu.VMEM((PER * capacity, d_model), BF16), pltpu.VMEM((SETS, PER * capacity, d_model), BF16),
                    pltpu.VMEM((PER * capacity, d_model), F32),
                    pltpu.VMEM((ns, d_model, FTILE), BF16), pltpu.VMEM((ns, FTILE, d_model), BF16),
                    pltpu.VMEM((GROUP, E_LOC + 8, 128), F32), pltpu.VMEM((GROUP, E_LOC + 8, 128), F32),
                    pltpu.VMEM((8, n_tok), F32), pltpu.VMEM((n_tok, 128), F32),
                    pltpu.VMEM((nc, 8, ROWS), F32), pltpu.VMEM((nc, ROWS, 128), F32),
                    dma(()), dma((GROUP,)), dma((GROUP,)),
                    dma((nc, GROUP)), dma((nc, GROUP)), dma((nc, GROUP)), dma((nc, GROUP)), dma((ns,)), dma((ns,)),
                ],
                compiler_params=pltpu.CompilerParams(
                    collective_id=number, has_side_effects=True, vmem_limit_bytes=66_000_000),
                name='moe_' + str(nc),
            )(*args)

        got, flag = moe(FAST, 0)
        got = lax.cond(flag[0, 0] > 0.0, lambda: moe(SAFE, 1)[0], lambda: got)
        return (x_loc.astype(F32) + gate_loc * got.astype(F32)).astype(BF16)

    tok_spec = P(('dp', 'ep2', 'ep'), None)
    w_spec = P(dev_axes, None, None)
    return jax.shard_map(local_step, mesh=mesh, in_specs=(tok_spec, tok_spec, tok_spec, w_spec, w_spec), out_specs=tok_spec, check_vma=False)
```

```python
import functools

import jax
import jax.numpy as jnp
from jax import lax
from jax.experimental import pallas as pl
from jax.experimental.pallas import tpu as pltpu
from jax.sharding import PartitionSpec as P

MESH = pl.DeviceIdType.MESH
F32 = jnp.float32
BF16 = jnp.bfloat16
GROUP = 8
EXPERTS = 128
E_LOC = EXPERTS // GROUP
SPAN = 512
Z = 32
ROWS = GROUP * Z
PER = 2
SETS = E_LOC // PER
FTILE = 1536
TTILE = 256
XTILE = 512
CTILE = 1024


def pick(values, i):
    out = values[0]
    for m in range(1, len(values)):
        out = out + (values[m] - values[m - 1]) * ((i + 16 - m) // 16)
    return out


class Plan:
    def __init__(self, lo, hi, slots, batches):
        self.lo, self.hi, self.slots = lo, hi, slots
        self.chunks = hi[-1]
        self.batches = batches
        assert sum(batches) in (self.chunks, self.chunks - 1)
        self.hi_before = (0,) + hi[:-1]
        self.lo_next = lo[1:] + (self.chunks,)
        self.pairs = tuple((h - l + 1) // 2 for l, h in zip(lo, hi))
        first = [min(m for m in range(SETS) if hi[m] > c) for c in range(self.chunks)]
        after = [max(m for m in range(SETS) if lo[m] <= c) + 1 for c in range(self.chunks)]
        self.wide = max(b - a for a, b in zip(first, after))
        self.first = tuple(min(m, SETS - self.wide) for m in first)
        assert all(h >= 2 * p for h, p in zip(hi, self.pairs))


FAST = Plan((0, 0, 2, 3, 4, 6, 7, 9), (2, 4, 6, 7, 8, 9, 11, 11), 5, (4, 4, 2))
SAFE = Plan((0,) * 8, (2, 4, 6, 8, 10, 12, 14, 16), 3, (4, 4, 4, 4))


def position():
    ep = lax.axis_index('ep')
    return lax.axis_index('ep2'), ep // 2, ep % 2


def partner(where, k):
    y, x, c = where
    py = (y + k // 4) % 2
    px = (x + (k // 2) % 2) % 2
    pc = (c + k % 2) % 2
    return py * 4 + px * 2 + pc, {'ep2': py, 'ep': px * 2 + pc}


def iota(shape, dim):
    return lax.broadcasted_iota(jnp.int32, shape, dim)


def hot(mask):
    return jnp.where(mask, 1.0, 0.0).astype(BF16)


def dot(a, b):
    return jnp.dot(a, b, preferred_element_type=F32)


def moe_kernel(plan, capacity, ids_ref, gate_ref, x_hbm, w_in, w_out, y_hbm, tail_ref, cols_hbm, flag_ref,
               xv, got, send, recv, rrecv, bbuf, obuf, acc, wi, wo, xbuf, cbuf, qrow, qcol, dlc, drc,
               x_sem, y_sem, c_sem, n_send, n_recv, s_send, s_recv, r_send, r_recv, wi_sem, wo_sem):
    nc, ns = plan.chunks, plan.slots
    n_tok, d_model = xv.shape
    per_e = w_in.shape[2] // FTILE
    slots = PER * capacity
    where = position()
    me = partner(where, 0)[0]

    def w_copies(i, slot):
        e, f = i // per_e, i % per_e
        cols = pl.ds(pl.multiple_of(f * FTILE, FTILE), FTILE)
        return (pltpu.make_async_copy(w_in.at[e, :, cols], wi.at[slot], wi_sem.at[slot]),
                pltpu.make_async_copy(w_out.at[e, cols, :], wo.at[slot], wo_sem.at[slot]))

    def x_copy(q):
        at = pl.ds(q * XTILE, XTILE)
        return pltpu.make_async_copy(x_hbm.at[at, :], xv.at[at, :], x_sem.at[q])

    def y_copy(t):
        at = pl.ds(pl.multiple_of(t * TTILE, TTILE), TTILE)
        return pltpu.make_async_copy(got.at[at, :], y_hbm.at[at, :], y_sem.at[t])

    def remote(src, dst, sent, received, k):
        return pltpu.make_async_remote_copy(src_ref=src, dst_ref=dst, send_sem=sent, recv_sem=received,
                                            device_id=partner(where, k)[1], device_id_type=MESH)

    def count_copy(k):
        return remote(xbuf.at[k], cbuf.at[k], n_send.at[k], n_recv.at[k], k)

    def out_copy(c, k):
        return remote(send.at[c, k], recv.at[c, k], s_send.at[c, k], s_recv.at[c, k], k)

    def back_copy(c, k):
        return remote(send.at[c, k], rrecv.at[c, k], r_send.at[c, k], r_recv.at[c, k], k)

    barrier = pltpu.get_barrier_semaphore()
    for k in range(1, GROUP):
        pl.semaphore_signal(barrier, inc=1, device_id=partner(where, k)[1], device_id_type=MESH)
    for q in range(n_tok // XTILE):
        x_copy(q).start()

    obuf[...] = jnp.zeros_like(obuf)

    row, col = iota((EXPERTS, EXPERTS), 0), iota((EXPERTS, EXPERTS), 1)
    same = (row // E_LOC) == (col // E_LOC)
    in_row, in_col = (row % E_LOC) // PER, (col % E_LOC) // PER
    inner = hot(same & (in_row == in_col) & (col < row))
    sums = [hot(same & (in_col == g)) for g in range(SETS)]

    def starts(counts):
        counts = counts.astype(BF16)
        base = jnp.zeros((EXPERTS, EXPERTS), F32)
        mine, over = base, base
        for g in range(SETS):
            if g:
                base = jnp.maximum(base, float(plan.lo[g] * Z))
            mine = jnp.where(in_row == g, base, mine)
            base = base + dot(sums[g], counts)
            over = jnp.maximum(over, base - float(plan.hi[g] * Z))
        return mine + dot(inner, counts), over

    chosen = hot(iota((EXPERTS, n_tok), 0) == ids_ref[...])
    counts = dot(chosen, jnp.ones((n_tok, 128), BF16))
    start, over = starts(counts)
    to_k = jnp.bitwise_xor(row // E_LOC, me).astype(F32)
    code0 = to_k * float(SPAN) + start

    upper = hot((iota((TTILE, TTILE + 128), 0) < iota((TTILE, TTILE + 128), 1)) | (iota((TTILE, TTILE + 128), 1) >= TTILE))
    base = code0
    for b in range(n_tok // TTILE):
        part = chosen[:, b * TTILE:(b + 1) * TTILE]
        rank = dot(part, upper)
        full = jnp.concatenate([rank[:, i * 128:(i + 1) * 128] + base for i in range(TTILE // 128)], axis=1)
        code = jnp.sum(part.astype(F32) * full, axis=0, keepdims=True)
        qrow[:, b * TTILE:(b + 1) * TTILE] = jnp.broadcast_to(code, (8, TTILE))
        base = base + rank[:, TTILE:]

    worst = jnp.broadcast_to(jnp.max(over, keepdims=True), (8, 128))
    acc[0:EXPERTS, 0:128] = counts
    for k in range(GROUP):
        at = pl.ds(pl.multiple_of(partner(where, k)[0] * E_LOC, E_LOC), E_LOC)
        xbuf[k, 0:E_LOC, :] = acc[at, 0:128]
        xbuf[k, E_LOC:E_LOC + 8, :] = worst
    cbuf[0] = xbuf[0]

    def targets(shape, dim):
        i = iota(shape, dim)
        k = jnp.zeros(shape, jnp.int32)
        c = k
        for m in range(1, -(-shape[dim] // ROWS)):
            c = c + jnp.where(i >= m * ROWS, 1, 0)
        i = i - c * ROWS
        for m in range(1, GROUP):
            k = k + jnp.where(i >= m * Z, 1, 0)
        return (i + k * (SPAN - Z) + c * Z).astype(F32)

    tcol = targets((ROWS, 1), 0)
    trow = targets((1, 4 * ROWS), 1)

    pl.semaphore_wait(barrier, GROUP - 1)
    for k in range(1, GROUP):
        count_copy(k).start()
    def send_out(c):
        for k in range(GROUP - 1, 0, -1):
            out_copy(c, k).start()
        recv[c, 0] = send[c, 0]

    packed = jnp.zeros((ROWS, d_model), F32)
    for q in range(n_tok // XTILE):
        x_copy(q).wait()
        at = slice(q * XTILE, (q + 1) * XTILE)
        packed = packed + dot(hot(tcol == qrow[0:1, at]), xv[at, :])
    send[0] = packed.astype(BF16).reshape(GROUP, Z, d_model)
    send_out(0)

    for i in range(ns):
        for copy in w_copies(i, i):
            copy.start()

    @pl.loop(1, nc)
    def _(c):
        mask = (tcol + (c * Z).astype(F32)) == qrow[0:1, :]
        send[c] = dot(hot(mask), xv[...]).astype(BF16).reshape(GROUP, Z, d_model)
        send_out(c)

    for b in range(n_tok // TTILE):
        at = slice(b * TTILE, (b + 1) * TTILE)
        both = jnp.where(iota((128, TTILE), 0) == 0, qrow[0:1, at], gate_ref[0:1, at])
        qcol[at, :] = jnp.transpose(both)
    c_copy = pltpu.make_async_copy(qcol, cols_hbm, c_sem)
    c_copy.start()
    for k in range(1, GROUP):
        count_copy(k).wait_recv()
    flag_ref[0, 0] = jnp.max(cbuf[:, E_LOC:E_LOC + 8, :])
    got_counts = cbuf[:, 0:E_LOC, :].reshape(EXPERTS, 128)
    start, _ = starts(got_counts)
    earlier = hot(((row % E_LOC) == (col % E_LOC)) & (jnp.bitwise_xor(col // E_LOC, me) < jnp.bitwise_xor(row // E_LOC, me)))
    ahead = dot(earlier, got_counts.astype(BF16))
    first = ((row // E_LOC) * SPAN).astype(F32) + start
    kept = jnp.minimum(got_counts, jnp.maximum(capacity - ahead, 0.0))
    last = first + kept
    shift = ((row % E_LOC) * capacity + 1).astype(F32) + ahead - first
    first, last, shift = first[:, 0:1], last[:, 0:1], shift[:, 0:1]
    for c in range(nc):
        at = trow[:, 0:ROWS] + float(c * Z)
        slot = jnp.sum(jnp.where((at >= first) & (at < last), at + shift, 0.0), axis=0, keepdims=True) - 1.0
        dlc[c] = jnp.broadcast_to(slot, (8, ROWS))
        drc[c] = jnp.transpose(jnp.broadcast_to(slot, (128, ROWS)))

    slot_col = iota((slots, 1), 0).astype(F32)
    slot_row = iota((1, plan.wide * slots), 1).astype(F32)

    @pl.loop(0, SETS)
    def _(g):
        @pl.loop(pick(plan.hi_before, g), pick(plan.hi, g))
        def _(c):
            for k in range(1, GROUP):
                out_copy(c, k).wait_recv()

        acc[...] = jnp.zeros_like(acc)

        @pl.loop(0, pick(plan.pairs, g))
        def _(p):
            c = pick(plan.hi, g) - 2 * p - 2
            slot = jnp.concatenate([dlc[c, 0:1, :], dlc[c + 1, 0:1, :]], axis=1)
            mask = (slot_col + (g * slots).astype(F32)) == slot
            acc[...] += dot(hot(mask), recv[pl.ds(c, 2)].reshape(2 * ROWS, d_model))

        bbuf[...] = acc[...].astype(BF16)

        @pl.loop(0, PER)
        def _(j):
            at = pl.ds(pl.multiple_of(j * capacity, capacity), capacity)
            first_i = (g * PER + j) * per_e
            total = None
            for f in range(per_e):
                i = first_i + f
                slot = i % ns
                for copy in w_copies(i, slot):
                    copy.wait()
                v = dot(bbuf[at, :], wi[slot])
                u = v * (0.7978845608028654 + (0.7978845608028654 * 0.044715) * (v * v))
                half = 0.5 * v
                part = dot((half + half * jnp.tanh(u)).astype(BF16), wo[slot])
                total = part if total is None else total + part

                @pl.when(i + ns < E_LOC * per_e)
                def _():
                    for copy in w_copies(i + ns, slot):
                        copy.start()
            obuf[g, at, :] = total.astype(BF16)

        @pl.loop(pick(plan.lo, g), pick(plan.lo_next, g))
        def _(c):
            m = pick(plan.first, c)
            mask = drc[c, :, 0:1] == (slot_row + (m * slots).astype(F32))
            packed = dot(hot(mask), obuf[pl.ds(m, plan.wide)].reshape(plan.wide * slots, d_model)).astype(BF16)
            for k in range(1, GROUP):
                out_copy(c, k).wait_send()
            send[c] = packed.reshape(GROUP, Z, d_model)
            for k in range(GROUP - 1, 0, -1):
                back_copy(c, k).start()
            rrecv[c, 0] = send[c, 0]

    def combine(c, count, fresh, finish):
        want = trow[:, 0:count * ROWS] + float(c * Z)
        for m in range(count):
            for k in range(1, GROUP):
                back_copy(c + m, k).wait_recv()

        @pl.loop(0, n_tok // TTILE)
        def _(t):
            at = pl.ds(pl.multiple_of(t * TTILE, TTILE), TTILE)
            rows = rrecv[c:c + count].reshape(count * ROWS, d_model)
            new = dot(hot(qcol[at, 0:1] == want), rows)
            if not fresh:
                new = got[at, :].astype(F32) + new
            if finish:
                new = xv[at, :].astype(F32) + qcol[at, 1:2] * new
            got[at, :] = new.astype(BF16)
            if finish:
                y_copy(t).start()

    c = 0
    for count in plan.batches:
        combine(c, count, c == 0, c + count == sum(plan.batches))
        c += count

    if c < nc:
        for k in range(1, GROUP):
            back_copy(c, k).wait_recv()
    tail_ref[...] = rrecv[nc - 1]

    for k in range(1, GROUP):
        count_copy(k).wait_send()

    @pl.loop(0, nc)
    def _(c):
        for k in range(1, GROUP):
            back_copy(c, k).wait_send()

    c_copy.wait()
    for t in range(n_tok // TTILE):
        y_copy(t).wait()


def close_kernel(shift, y1_ref, tail_ref, cols_ref, y_ref):
    i = iota((1, ROWS), 1)
    want = ((i // Z) * (SPAN - Z) + i + shift).astype(F32)
    new = dot(hot(cols_ref[:, 0:1] == want), tail_ref[...])
    y_ref[...] = (y1_ref[...].astype(F32) + cols_ref[:, 1:2] * new).astype(BF16)


def solution(mesh):
    dev_axes = ('ep2', 'ep')

    def local_step(x_loc, ids_loc, gate_loc, w_a, w_b):
        n_tok, d_model = x_loc.shape
        capacity = 8 * ((5 * GROUP * n_tok) // (32 * EXPERTS))
        vmem = pl.BlockSpec(memory_space=pltpu.VMEM)
        hbm = pl.BlockSpec(memory_space=pl.ANY)
        dma = pltpu.SemaphoreType.DMA
        gate_row = gate_loc.reshape(1, n_tok)
        args = (ids_loc.reshape(1, n_tok), gate_row, x_loc, w_a, w_b)

        def moe(plan, number):
            nc, ns = plan.chunks, plan.slots
            block = pltpu.VMEM((nc, GROUP, Z, d_model), BF16)
            return pl.pallas_call(
                functools.partial(moe_kernel, plan, capacity),
                out_shape=(jax.ShapeDtypeStruct((n_tok, d_model), BF16), jax.ShapeDtypeStruct((GROUP, Z, d_model), BF16),
                           jax.ShapeDtypeStruct((n_tok, 128), F32), jax.ShapeDtypeStruct((1, 1), F32)),
                in_specs=[vmem] * 2 + [hbm] * 3, out_specs=(hbm, vmem, hbm, pl.BlockSpec(memory_space=pltpu.SMEM)),
                scratch_shapes=[
                    pltpu.VMEM((n_tok, d_model), BF16), pltpu.VMEM((n_tok, d_model), BF16),
                    block, block, block,
                    pltpu.VMEM((PER * capacity, d_model), BF16), pltpu.VMEM((SETS, PER * capacity, d_model), BF16),
                    pltpu.VMEM((PER * capacity, d_model), F32),
                    pltpu.VMEM((ns, d_model, FTILE), BF16), pltpu.VMEM((ns, FTILE, d_model), BF16),
                    pltpu.VMEM((GROUP, E_LOC + 8, 128), F32), pltpu.VMEM((GROUP, E_LOC + 8, 128), F32),
                    pltpu.VMEM((8, n_tok), F32), pltpu.VMEM((n_tok, 128), F32),
                    pltpu.VMEM((nc, 8, ROWS), F32), pltpu.VMEM((nc, ROWS, 128), F32),
                    dma((n_tok // XTILE,)), dma((n_tok // TTILE,)), dma(()), dma((GROUP,)), dma((GROUP,)),
                    dma((nc, GROUP)), dma((nc, GROUP)), dma((nc, GROUP)), dma((nc, GROUP)), dma((ns,)), dma((ns,)),
                ],
                compiler_params=pltpu.CompilerParams(
                    collective_id=number, has_side_effects=True, vmem_limit_bytes=66_000_000),
                name='moe_' + str(nc),
            )(*args)

        y1, tail, cols, flag = moe(FAST, 0)
        y1, tail = lax.cond(flag[0, 0] > 0.0, lambda: (moe(SAFE, 1)[0], jnp.zeros_like(tail)), lambda: (y1, tail))
        rows = lambda width: pl.BlockSpec((CTILE, width), lambda t: (t, 0))
        return pl.pallas_call(
            functools.partial(close_kernel, (FAST.chunks - 1) * Z),
            out_shape=jax.ShapeDtypeStruct((n_tok, d_model), BF16), grid=(n_tok // CTILE,),
            in_specs=[rows(d_model), pl.BlockSpec((ROWS, d_model), lambda t: (0, 0)), rows(128)], out_specs=rows(d_model),
            name='close',
        )(y1, tail.reshape(ROWS, d_model), cols)

    tok_spec = P(('dp', 'ep2', 'ep'), None)
    w_spec = P(dev_axes, None, None)
    return jax.shard_map(local_step, mesh=mesh, in_specs=(tok_spec, tok_spec, tok_spec, w_spec, w_spec), out_specs=tok_spec, check_vma=False)
```

```python
import functools

import jax
import jax.numpy as jnp
from jax import lax
from jax.experimental import pallas as pl
from jax.experimental.pallas import tpu as pltpu
from jax.sharding import PartitionSpec as P

MESH = pl.DeviceIdType.MESH
F32 = jnp.float32
BF16 = jnp.bfloat16
GROUP = 8
EXPERTS = 128
E_LOC = EXPERTS // GROUP
SPAN = 512
Z = 32
ROWS = GROUP * Z
PER = 2
SETS = E_LOC // PER
FTILE = 1536
TTILE = 256
XTILE = 512
CTILE = 1024


def pick(values, i):
    out = values[0]
    for m in range(1, len(values)):
        out = out + (values[m] - values[m - 1]) * ((i + 16 - m) // 16)
    return out


class Plan:
    def __init__(self, lo, hi, slots, batches, shared):
        self.lo, self.hi, self.slots, self.shared = lo, hi, slots, shared
        self.places = hi[-1]
        self.chunks = self.places - shared
        self.batches = batches
        assert sum(batches) in (self.chunks, self.chunks - 1)
        self.hi_before = (0,) + hi[:-1]
        self.lo_next = lo[1:] + (self.chunks - shared,)
        assert all(a <= b for a, b in zip(lo, self.lo_next))
        self.pairs = tuple((h - l + 1) // 2 for l, h in zip(lo, hi))
        first = [min(m for m in range(SETS) if hi[m] > c) for c in range(self.places)]
        after = [max(m for m in range(SETS) if lo[m] <= c) + 1 for c in range(self.places)]
        self.wide = max(b - a for a, b in zip(first, after))
        self.first = tuple(min(m, SETS - self.wide) for m in first)
        assert all(h >= 2 * p for h, p in zip(hi, self.pairs))


FAST = Plan((0, 0, 1, 2, 3, 5, 6, 7), (2, 4, 6, 7, 8, 9, 10, 11), 5, (4, 4, 1), 1)
SAFE = Plan((0,) * 8, (2, 4, 6, 8, 10, 12, 14, 16), 3, (4, 4, 4, 4), 0)


def position():
    ep = lax.axis_index('ep')
    return lax.axis_index('ep2'), ep // 2, ep % 2


def partner(where, k):
    y, x, c = where
    py = (y + k // 4) % 2
    px = (x + (k // 2) % 2) % 2
    pc = (c + k % 2) % 2
    return py * 4 + px * 2 + pc, {'ep2': py, 'ep': px * 2 + pc}


def iota(shape, dim):
    return lax.broadcasted_iota(jnp.int32, shape, dim)


def hot(mask):
    return jnp.where(mask, 1.0, 0.0).astype(BF16)


def dot(a, b):
    return jnp.dot(a, b, preferred_element_type=F32)


def moe_kernel(plan, capacity, ids_ref, gate_ref, x_hbm, w_in, w_out, y_hbm, tail_ref, cols_hbm, flag_ref,
               xv, got, send, recv, rrecv, xsend, xrecv, bbuf, obuf, acc, wi, wo, xbuf, cbuf, qrow, qcol, dlc, drc,
               x_sem, y_sem, c_sem, n_send, n_recv, s_send, s_recv, r_send, r_recv, x_send, x_recv, wi_sem, wo_sem):
    nc, ns = plan.chunks, plan.slots
    n_tok, d_model = xv.shape
    per_e = w_in.shape[2] // FTILE
    slots = PER * capacity
    where = position()
    me = partner(where, 0)[0]

    def w_copies(i, slot):
        e, f = i // per_e, i % per_e
        cols = pl.ds(pl.multiple_of(f * FTILE, FTILE), FTILE)
        return (pltpu.make_async_copy(w_in.at[e, :, cols], wi.at[slot], wi_sem.at[slot]),
                pltpu.make_async_copy(w_out.at[e, cols, :], wo.at[slot], wo_sem.at[slot]))

    def x_copy(q):
        at = pl.ds(q * XTILE, XTILE)
        return pltpu.make_async_copy(x_hbm.at[at, :], xv.at[at, :], x_sem.at[q])

    def y_copy(t):
        at = pl.ds(pl.multiple_of(t * TTILE, TTILE), TTILE)
        return pltpu.make_async_copy(got.at[at, :], y_hbm.at[at, :], y_sem.at[t])

    def remote(src, dst, sent, received, k):
        return pltpu.make_async_remote_copy(src_ref=src, dst_ref=dst, send_sem=sent, recv_sem=received,
                                            device_id=partner(where, k)[1], device_id_type=MESH)

    def count_copy(k):
        return remote(xbuf.at[k], cbuf.at[k], n_send.at[k], n_recv.at[k], k)

    def out_copy(c, k):
        return remote(send.at[c, k], recv.at[c, k], s_send.at[c, k], s_recv.at[c, k], k)

    def pass_on():
        return remote(recv.at[nc - 1], recv.at[nc], x_send.at[0], x_recv.at[0], 1)

    def hand_over():
        return remote(xsend, xrecv, x_send.at[1], x_recv.at[1], 1)

    def back_copy(c, k):
        return remote(send.at[c, k], rrecv.at[c, k], r_send.at[c, k], r_recv.at[c, k], k)

    barrier = pltpu.get_barrier_semaphore()
    for k in range(1, GROUP):
        pl.semaphore_signal(barrier, inc=1, device_id=partner(where, k)[1], device_id_type=MESH)
    for q in range(n_tok // XTILE):
        x_copy(q).start()

    obuf[...] = jnp.zeros_like(obuf)

    row, col = iota((EXPERTS, EXPERTS), 0), iota((EXPERTS, EXPERTS), 1)
    same = (row // E_LOC) == (col // E_LOC)
    in_row, in_col = (row % E_LOC) // PER, (col % E_LOC) // PER
    inner = hot(same & (in_row == in_col) & (col < row))
    sums = [hot(same & (in_col == g)) for g in range(SETS)]

    def starts(counts):
        counts = counts.astype(BF16)
        base = jnp.zeros((EXPERTS, EXPERTS), F32)
        mine, over = base, base
        for g in range(SETS):
            if g:
                base = jnp.maximum(base, float(plan.lo[g] * Z))
            mine = jnp.where(in_row == g, base, mine)
            base = base + dot(sums[g], counts)
            over = jnp.maximum(over, base - float(plan.hi[g] * Z))
        if plan.shared:
            other = jnp.concatenate([base[(b ^ 1) * E_LOC:((b ^ 1) + 1) * E_LOC] for b in range(GROUP)], axis=0)
            over = jnp.maximum(over, base + other - float(2 * nc * Z))
        return mine + dot(inner, counts), over

    chosen = hot(iota((EXPERTS, n_tok), 0) == ids_ref[...])
    counts = dot(chosen, jnp.ones((n_tok, 128), BF16))
    start, over = starts(counts)
    to_k = jnp.bitwise_xor(row // E_LOC, me).astype(F32)
    code0 = to_k * float(SPAN) + start

    upper = hot((iota((TTILE, TTILE + 128), 0) < iota((TTILE, TTILE + 128), 1)) | (iota((TTILE, TTILE + 128), 1) >= TTILE))
    base = code0
    for b in range(n_tok // TTILE):
        part = chosen[:, b * TTILE:(b + 1) * TTILE]
        rank = dot(part, upper)
        full = jnp.concatenate([rank[:, i * 128:(i + 1) * 128] + base for i in range(TTILE // 128)], axis=1)
        code = jnp.sum(part.astype(F32) * full, axis=0, keepdims=True)
        if plan.shared:
            whole = code.astype(jnp.int32)
            k, place = whole // SPAN, whole % SPAN
            mirrored = jnp.bitwise_xor(k, 1) * SPAN + (2 * nc * Z - 1) - place
            code = jnp.where(place >= nc * Z, mirrored, whole).astype(F32)
        qrow[:, b * TTILE:(b + 1) * TTILE] = jnp.broadcast_to(code, (8, TTILE))
        base = base + rank[:, TTILE:]

    worst = jnp.broadcast_to(jnp.max(over, keepdims=True), (8, 128))
    acc[0:EXPERTS, 0:128] = counts
    for k in range(GROUP):
        at = pl.ds(pl.multiple_of(partner(where, k)[0] * E_LOC, E_LOC), E_LOC)
        xbuf[k, 0:E_LOC, :] = acc[at, 0:128]
        xbuf[k, E_LOC:E_LOC + 8, :] = worst
    cbuf[0] = xbuf[0]

    def targets(shape, dim):
        i = iota(shape, dim)
        k = jnp.zeros(shape, jnp.int32)
        c = k
        for m in range(1, -(-shape[dim] // ROWS)):
            c = c + jnp.where(i >= m * ROWS, 1, 0)
        i = i - c * ROWS
        for m in range(1, GROUP):
            k = k + jnp.where(i >= m * Z, 1, 0)
        return (i + k * (SPAN - Z) + c * Z).astype(F32)

    tcol = targets((ROWS, 1), 0)
    trow = targets((1, 4 * ROWS), 1)

    pl.semaphore_wait(barrier, GROUP - 1)
    for k in range(1, GROUP):
        count_copy(k).start()
    def send_out(c):
        for k in range(GROUP - 1, 0, -1):
            out_copy(c, k).start()
        recv[c, 0] = send[c, 0]

    packed = jnp.zeros((ROWS, d_model), F32)
    for q in range(n_tok // XTILE):
        x_copy(q).wait()
        at = slice(q * XTILE, (q + 1) * XTILE)
        packed = packed + dot(hot(tcol == qrow[0:1, at]), xv[at, :])
    send[0] = packed.astype(BF16).reshape(GROUP, Z, d_model)
    send_out(0)

    for i in range(ns):
        for copy in w_copies(i, i):
            copy.start()

    @pl.loop(1, nc)
    def _(c):
        mask = (tcol + (c * Z).astype(F32)) == qrow[0:1, :]
        send[c] = dot(hot(mask), xv[...]).astype(BF16).reshape(GROUP, Z, d_model)
        send_out(c)

    for b in range(n_tok // TTILE):
        at = slice(b * TTILE, (b + 1) * TTILE)
        both = jnp.where(iota((128, TTILE), 0) == 0, qrow[0:1, at], gate_ref[0:1, at])
        qcol[at, :] = jnp.transpose(both)
    c_copy = pltpu.make_async_copy(qcol, cols_hbm, c_sem)
    c_copy.start()
    for k in range(1, GROUP):
        count_copy(k).wait_recv()
    flag_ref[0, 0] = jnp.max(cbuf[:, E_LOC:E_LOC + 8, :])
    got_counts = cbuf[:, 0:E_LOC, :].reshape(EXPERTS, 128)
    start, _ = starts(got_counts)
    earlier = hot(((row % E_LOC) == (col % E_LOC)) & (jnp.bitwise_xor(col // E_LOC, me) < jnp.bitwise_xor(row // E_LOC, me)))
    ahead = dot(earlier, got_counts.astype(BF16))
    first = ((row // E_LOC) * SPAN).astype(F32) + start
    kept = jnp.minimum(got_counts, jnp.maximum(capacity - ahead, 0.0))
    last = first + kept
    shift = ((row % E_LOC) * capacity + 1).astype(F32) + ahead - first
    first, last, shift = first[:, 0:1], last[:, 0:1], shift[:, 0:1]
    lane = iota((1, ROWS), 1)
    for c in range(plan.places):
        if c < nc:
            at = trow[:, 0:ROWS] + float(c * Z)
        else:
            at = (jnp.bitwise_xor(lane // Z, 1) * SPAN + (2 * nc * Z - 1 - (nc - 1) * Z) - lane % Z).astype(F32)
        slot = jnp.sum(jnp.where((at >= first) & (at < last), at + shift, 0.0), axis=0, keepdims=True) - 1.0
        dlc[c] = jnp.broadcast_to(slot, (8, ROWS))
        drc[c] = jnp.transpose(jnp.broadcast_to(slot, (128, ROWS)))

    slot_col = iota((slots, 1), 0).astype(F32)
    slot_row = iota((1, plan.wide * slots), 1).astype(F32)

    def pack(c, m):
        mask = drc[c, :, 0:1] == (slot_row + m * float(slots) if isinstance(m, int) else slot_row + (m * slots).astype(F32))
        packed = dot(hot(mask), obuf[pl.ds(m, plan.wide)].reshape(plan.wide * slots, d_model))
        return packed.astype(BF16).reshape(GROUP, Z, d_model)

    def send_back(c, packed):
        for k in range(1, GROUP):
            out_copy(c, k).wait_send()
        send[c] = packed
        for k in range(GROUP - 1, 0, -1):
            back_copy(c, k).start()
        rrecv[c, 0] = send[c, 0]

    @pl.loop(0, SETS)
    def _(g):
        @pl.loop(pick(plan.hi_before, g), pick(plan.hi, g))
        def _(c):
            @pl.when(c < nc)
            def _():
                for k in range(1, GROUP):
                    out_copy(c, k).wait_recv()

            if plan.shared:
                @pl.when(c == nc - 1)
                def _():
                    pass_on().start()

                @pl.when(c == nc)
                def _():
                    pass_on().wait_recv()

        acc[...] = jnp.zeros_like(acc)

        @pl.loop(0, pick(plan.pairs, g))
        def _(p):
            c = pick(plan.hi, g) - 2 * p - 2
            slot = jnp.concatenate([dlc[c, 0:1, :], dlc[c + 1, 0:1, :]], axis=1)
            mask = (slot_col + (g * slots).astype(F32)) == slot
            acc[...] += dot(hot(mask), recv[pl.ds(c, 2)].reshape(2 * ROWS, d_model))

        bbuf[...] = acc[...].astype(BF16)

        @pl.loop(0, PER)
        def _(j):
            at = pl.ds(pl.multiple_of(j * capacity, capacity), capacity)
            first_i = (g * PER + j) * per_e
            total = None
            for f in range(per_e):
                i = first_i + f
                slot = i % ns
                for copy in w_copies(i, slot):
                    copy.wait()
                v = dot(bbuf[at, :], wi[slot])
                u = v * (0.7978845608028654 + (0.7978845608028654 * 0.044715) * (v * v))
                half = 0.5 * v
                part = dot((half + half * jnp.tanh(u)).astype(BF16), wo[slot])
                total = part if total is None else total + part

                @pl.when(i + ns < E_LOC * per_e)
                def _():
                    for copy in w_copies(i + ns, slot):
                        copy.start()
            obuf[g, at, :] = total.astype(BF16)

        @pl.loop(pick(plan.lo, g), pick(plan.lo_next, g))
        def _(c):
            send_back(c, pack(c, pick(plan.first, c)))

    if plan.shared:
        xsend[...] = pack(nc, plan.first[nc])
        hand_over().start()
        packed = pack(nc - 1, plan.first[nc - 1])
        hand_over().wait_recv()
        send_back(nc - 1, packed + xrecv[...])

    def combine(c, count, fresh, finish):
        want = trow[:, 0:count * ROWS] + float(c * Z)
        for m in range(count):
            for k in range(1, GROUP):
                back_copy(c + m, k).wait_recv()

        @pl.loop(0, n_tok // TTILE)
        def _(t):
            at = pl.ds(pl.multiple_of(t * TTILE, TTILE), TTILE)
            rows = rrecv[c:c + count].reshape(count * ROWS, d_model)
            new = dot(hot(qcol[at, 0:1] == want), rows)
            if not fresh:
                new = got[at, :].astype(F32) + new
            if finish:
                new = xv[at, :].astype(F32) + qcol[at, 1:2] * new
            got[at, :] = new.astype(BF16)
            if finish:
                y_copy(t).start()

    c = 0
    for count in plan.batches:
        combine(c, count, c == 0, c + count == sum(plan.batches))
        c += count

    if c < nc:
        for k in range(1, GROUP):
            back_copy(c, k).wait_recv()
    tail_ref[...] = rrecv[nc - 1]

    for k in range(1, GROUP):
        count_copy(k).wait_send()
    if plan.shared:
        pass_on().wait_send()
        hand_over().wait_send()

    @pl.loop(0, nc)
    def _(c):
        for k in range(1, GROUP):
            back_copy(c, k).wait_send()

    c_copy.wait()
    for t in range(n_tok // TTILE):
        y_copy(t).wait()


def close_kernel(shift, y1_ref, tail_ref, cols_ref, y_ref):
    i = iota((1, ROWS), 1)
    want = ((i // Z) * (SPAN - Z) + i + shift).astype(F32)
    new = dot(hot(cols_ref[:, 0:1] == want), tail_ref[...])
    y_ref[...] = (y1_ref[...].astype(F32) + cols_ref[:, 1:2] * new).astype(BF16)


def solution(mesh):
    dev_axes = ('ep2', 'ep')

    def local_step(x_loc, ids_loc, gate_loc, w_a, w_b):
        n_tok, d_model = x_loc.shape
        capacity = 8 * ((5 * GROUP * n_tok) // (32 * EXPERTS))
        vmem = pl.BlockSpec(memory_space=pltpu.VMEM)
        hbm = pl.BlockSpec(memory_space=pl.ANY)
        dma = pltpu.SemaphoreType.DMA
        gate_row = gate_loc.reshape(1, n_tok)
        args = (ids_loc.reshape(1, n_tok), gate_row, x_loc, w_a, w_b)

        def moe(plan, number):
            nc, ns = plan.chunks, plan.slots
            block = pltpu.VMEM((nc, GROUP, Z, d_model), BF16)
            chunk = pltpu.VMEM((GROUP, Z, d_model), BF16)
            return pl.pallas_call(
                functools.partial(moe_kernel, plan, capacity),
                out_shape=(jax.ShapeDtypeStruct((n_tok, d_model), BF16), jax.ShapeDtypeStruct((GROUP, Z, d_model), BF16),
                           jax.ShapeDtypeStruct((n_tok, 128), F32), jax.ShapeDtypeStruct((1, 1), F32)),
                in_specs=[vmem] * 2 + [hbm] * 3, out_specs=(hbm, vmem, hbm, pl.BlockSpec(memory_space=pltpu.SMEM)),
                scratch_shapes=[
                    pltpu.VMEM((n_tok, d_model), BF16), pltpu.VMEM((n_tok, d_model), BF16),
                    block, pltpu.VMEM((plan.places, GROUP, Z, d_model), BF16), block, chunk, chunk,
                    pltpu.VMEM((PER * capacity, d_model), BF16), pltpu.VMEM((SETS, PER * capacity, d_model), BF16),
                    pltpu.VMEM((PER * capacity, d_model), F32),
                    pltpu.VMEM((ns, d_model, FTILE), BF16), pltpu.VMEM((ns, FTILE, d_model), BF16),
                    pltpu.VMEM((GROUP, E_LOC + 8, 128), F32), pltpu.VMEM((GROUP, E_LOC + 8, 128), F32),
                    pltpu.VMEM((8, n_tok), F32), pltpu.VMEM((n_tok, 128), F32),
                    pltpu.VMEM((plan.places, 8, ROWS), F32), pltpu.VMEM((plan.places, ROWS, 128), F32),
                    dma((n_tok // XTILE,)), dma((n_tok // TTILE,)), dma(()), dma((GROUP,)), dma((GROUP,)),
                    dma((nc, GROUP)), dma((nc, GROUP)), dma((nc, GROUP)), dma((nc, GROUP)), dma((2,)), dma((2,)), dma((ns,)), dma((ns,)),
                ],
                compiler_params=pltpu.CompilerParams(
                    collective_id=number, has_side_effects=True, vmem_limit_bytes=66_000_000),
                name='moe_' + str(nc),
            )(*args)

        y1, tail, cols, flag = moe(FAST, 0)
        y1, tail = lax.cond(flag[0, 0] > 0.0, lambda: (moe(SAFE, 1)[0], jnp.zeros_like(tail)), lambda: (y1, tail))
        rows = lambda width: pl.BlockSpec((CTILE, width), lambda t: (t, 0))
        return pl.pallas_call(
            functools.partial(close_kernel, (FAST.chunks - 1) * Z),
            out_shape=jax.ShapeDtypeStruct((n_tok, d_model), BF16), grid=(n_tok // CTILE,),
            in_specs=[rows(d_model), pl.BlockSpec((ROWS, d_model), lambda t: (0, 0)), rows(128)], out_specs=rows(d_model),
            name='close',
        )(y1, tail.reshape(ROWS, d_model), cols)

    tok_spec = P(('dp', 'ep2', 'ep'), None)
    w_spec = P(dev_axes, None, None)
    return jax.shard_map(local_step, mesh=mesh, in_specs=(tok_spec, tok_spec, tok_spec, w_spec, w_spec), out_specs=tok_spec, check_vma=False)
```

```python
import functools

import jax
import jax.numpy as jnp
from jax import lax
from jax.experimental import pallas as pl
from jax.experimental.pallas import tpu as pltpu
from jax.sharding import PartitionSpec as P

MESH = pl.DeviceIdType.MESH
F32 = jnp.float32
BF16 = jnp.bfloat16
GROUP = 8
EXPERTS = 128
E_LOC = EXPERTS // GROUP
SPAN = 512
Z = 32
ROWS = GROUP * Z
PER = 2
SETS = E_LOC // PER
FTILE = 1536
TTILE = 256
XTILE = 2048
CTILE = 1024


def pick(values, i):
    out = values[0]
    for m in range(1, len(values)):
        out = out + (values[m] - values[m - 1]) * ((i + 16 - m) // 16)
    return out


class Plan:
    def __init__(self, lo, hi, slots, batches, shared):
        self.lo, self.hi, self.slots, self.shared = lo, hi, slots, shared
        self.places = hi[-1]
        self.chunks = self.places - shared
        self.batches = batches
        assert sum(batches) in (self.chunks, self.chunks - 1)
        self.hi_before = (0,) + hi[:-1]
        self.lo_next = lo[1:] + (self.chunks - shared,)
        assert all(a <= b for a, b in zip(lo, self.lo_next))
        self.pairs = tuple((h - l + 1) // 2 for l, h in zip(lo, hi))
        first = [min(m for m in range(SETS) if hi[m] > c) for c in range(self.places)]
        after = [max(m for m in range(SETS) if lo[m] <= c) + 1 for c in range(self.places)]
        self.wide = max(b - a for a, b in zip(first, after))
        self.first = tuple(min(m, SETS - self.wide) for m in first)
        assert all(h >= 2 * p for h, p in zip(hi, self.pairs))


FAST = Plan((0, 0, 1, 2, 3, 5, 6, 7), (2, 4, 6, 7, 8, 9, 10, 11), 5, (4, 4, 1), 1)
SAFE = Plan((0,) * 8, (2, 4, 6, 8, 10, 12, 14, 16), 3, (4, 4, 4, 4), 0)


def position():
    ep = lax.axis_index('ep')
    return lax.axis_index('ep2'), ep // 2, ep % 2


def partner(where, k):
    y, x, c = where
    py = (y + k // 4) % 2
    px = (x + (k // 2) % 2) % 2
    pc = (c + k % 2) % 2
    return py * 4 + px * 2 + pc, {'ep2': py, 'ep': px * 2 + pc}


def iota(shape, dim):
    return lax.broadcasted_iota(jnp.int32, shape, dim)


def hot(mask):
    return jnp.where(mask, 1.0, 0.0).astype(BF16)


def dot(a, b):
    return jnp.dot(a, b, preferred_element_type=F32)


def moe_kernel(plan, capacity, ids_hbm, gate_hbm, x_hbm, w_in, w_out, y_hbm, tail_ref, cols_hbm, flag_hbm,
               ids_ref, gate_ref, flag_ref, xv, got, send, recv, rrecv, xsend, xrecv, bbuf, obuf, acc, wi, wo, xbuf, cbuf, qrow, qcol, dlc, drc,
               i_sem, x_sem, y_sem, c_sem, n_send, n_recv, s_send, s_recv, r_send, r_recv, x_send, x_recv, wi_sem, wo_sem):
    nc, ns = plan.chunks, plan.slots
    n_tok, d_model = xv.shape
    per_e = w_in.shape[2] // FTILE
    slots = PER * capacity
    where = position()
    me = partner(where, 0)[0]

    def w_copies(i, slot):
        e, f = i // per_e, i % per_e
        cols = pl.ds(pl.multiple_of(f * FTILE, FTILE), FTILE)
        return (pltpu.make_async_copy(w_in.at[e, :, cols], wi.at[slot], wi_sem.at[slot]),
                pltpu.make_async_copy(w_out.at[e, cols, :], wo.at[slot], wo_sem.at[slot]))

    def x_copy(q):
        at = pl.ds(q * XTILE, XTILE)
        return pltpu.make_async_copy(x_hbm.at[at, :], xv.at[at, :], x_sem.at[q])

    def y_copy(t):
        at = pl.ds(pl.multiple_of(t * TTILE, TTILE), TTILE)
        return pltpu.make_async_copy(got.at[at, :], y_hbm.at[at, :], y_sem.at[t])

    def remote(src, dst, sent, received, k):
        return pltpu.make_async_remote_copy(src_ref=src, dst_ref=dst, send_sem=sent, recv_sem=received,
                                            device_id=partner(where, k)[1], device_id_type=MESH)

    def count_copy(k):
        return remote(xbuf.at[k], cbuf.at[k], n_send.at[k], n_recv.at[k], k)

    def out_copy(c, k):
        return remote(send.at[c, k], recv.at[c, k], s_send.at[c, k], s_recv.at[c, k], k)

    def pass_on():
        return remote(recv.at[nc - 1], recv.at[nc], x_send.at[0], x_recv.at[0], 1)

    def hand_over():
        return remote(xsend, xrecv, x_send.at[1], x_recv.at[1], 1)

    def back_copy(c, k):
        return remote(send.at[c, k], rrecv.at[c, k], r_send.at[c, k], r_recv.at[c, k], k)

    ids_copy = pltpu.make_async_copy(ids_hbm, ids_ref, i_sem.at[0])
    gate_copy = pltpu.make_async_copy(gate_hbm, gate_ref, i_sem.at[1])
    flag_copy = pltpu.make_async_copy(flag_ref, flag_hbm, i_sem.at[2])
    ids_copy.start()
    gate_copy.start()
    barrier = pltpu.get_barrier_semaphore()
    for k in range(1, GROUP):
        pl.semaphore_signal(barrier, inc=1, device_id=partner(where, k)[1], device_id_type=MESH)
    for q in range(n_tok // XTILE):
        x_copy(q).start()

    obuf[...] = jnp.zeros_like(obuf)

    row, col = iota((EXPERTS, EXPERTS), 0), iota((EXPERTS, EXPERTS), 1)
    same = (row // E_LOC) == (col // E_LOC)
    in_row, in_col = (row % E_LOC) // PER, (col % E_LOC) // PER
    inner = hot(same & (in_row == in_col) & (col < row))
    sums = [hot(same & (in_col == g)) for g in range(SETS)]

    def starts(counts):
        counts = counts.astype(BF16)
        base = jnp.zeros((EXPERTS, EXPERTS), F32)
        mine, over = base, base
        for g in range(SETS):
            if g:
                base = jnp.maximum(base, float(plan.lo[g] * Z))
            mine = jnp.where(in_row == g, base, mine)
            base = base + dot(sums[g], counts)
            over = jnp.maximum(over, base - float(plan.hi[g] * Z))
        if plan.shared:
            other = jnp.concatenate([base[(b ^ 1) * E_LOC:((b ^ 1) + 1) * E_LOC] for b in range(GROUP)], axis=0)
            over = jnp.maximum(over, base + other - float(2 * nc * Z))
        return mine + dot(inner, counts), over

    ids_copy.wait()
    chosen = hot(iota((EXPERTS, n_tok), 0) == ids_ref[...])
    counts = dot(chosen, jnp.ones((n_tok, 128), BF16))
    start, over = starts(counts)
    to_k = jnp.bitwise_xor(row // E_LOC, me).astype(F32)
    code0 = to_k * float(SPAN) + start

    upper = hot((iota((TTILE, TTILE + 128), 0) < iota((TTILE, TTILE + 128), 1)) | (iota((TTILE, TTILE + 128), 1) >= TTILE))
    base = code0
    for b in range(n_tok // TTILE):
        part = chosen[:, b * TTILE:(b + 1) * TTILE]
        rank = dot(part, upper)
        full = jnp.concatenate([rank[:, i * 128:(i + 1) * 128] + base for i in range(TTILE // 128)], axis=1)
        code = jnp.sum(part.astype(F32) * full, axis=0, keepdims=True)
        if plan.shared:
            whole = code.astype(jnp.int32)
            k, place = whole // SPAN, whole % SPAN
            mirrored = jnp.bitwise_xor(k, 1) * SPAN + (2 * nc * Z - 1) - place
            code = jnp.where(place >= nc * Z, mirrored, whole).astype(F32)
        qrow[:, b * TTILE:(b + 1) * TTILE] = jnp.broadcast_to(code, (8, TTILE))
        base = base + rank[:, TTILE:]

    worst = jnp.broadcast_to(jnp.max(over, keepdims=True), (8, 128))
    acc[0:EXPERTS, 0:128] = counts
    for k in range(GROUP):
        at = pl.ds(pl.multiple_of(partner(where, k)[0] * E_LOC, E_LOC), E_LOC)
        xbuf[k, 0:E_LOC, :] = acc[at, 0:128]
        xbuf[k, E_LOC:E_LOC + 8, :] = worst
    cbuf[0] = xbuf[0]

    def targets(shape, dim):
        i = iota(shape, dim)
        k = jnp.zeros(shape, jnp.int32)
        c = k
        for m in range(1, -(-shape[dim] // ROWS)):
            c = c + jnp.where(i >= m * ROWS, 1, 0)
        i = i - c * ROWS
        for m in range(1, GROUP):
            k = k + jnp.where(i >= m * Z, 1, 0)
        return (i + k * (SPAN - Z) + c * Z).astype(F32)

    tcol = targets((ROWS, 1), 0)
    trow = targets((1, 4 * ROWS), 1)

    pl.semaphore_wait(barrier, GROUP - 1)
    for k in range(1, GROUP):
        count_copy(k).start()
    def send_out(c):
        for k in range(GROUP - 1, 0, -1):
            out_copy(c, k).start()
        recv[c, 0] = send[c, 0]

    packed = jnp.zeros((ROWS, d_model), F32)
    for q in range(n_tok // XTILE):
        x_copy(q).wait()
        at = slice(q * XTILE, (q + 1) * XTILE)
        packed = packed + dot(hot(tcol == qrow[0:1, at]), xv[at, :])
    send[0] = packed.astype(BF16).reshape(GROUP, Z, d_model)
    send_out(0)

    for i in range(ns):
        for copy in w_copies(i, i):
            copy.start()

    @pl.loop(1, nc)
    def _(c):
        mask = (tcol + (c * Z).astype(F32)) == qrow[0:1, :]
        send[c] = dot(hot(mask), xv[...]).astype(BF16).reshape(GROUP, Z, d_model)
        send_out(c)

    gate_copy.wait()
    for b in range(n_tok // TTILE):
        at = slice(b * TTILE, (b + 1) * TTILE)
        both = jnp.where(iota((128, TTILE), 0) == 0, qrow[0:1, at], gate_ref[0:1, at])
        qcol[at, :] = jnp.transpose(both)
    c_copy = pltpu.make_async_copy(qcol, cols_hbm, c_sem)
    c_copy.start()
    for k in range(1, GROUP):
        count_copy(k).wait_recv()
    flag_ref[0, 0] = jnp.max(cbuf[:, E_LOC:E_LOC + 8, :])
    flag_copy.start()
    got_counts = cbuf[:, 0:E_LOC, :].reshape(EXPERTS, 128)
    start, _ = starts(got_counts)
    earlier = hot(((row % E_LOC) == (col % E_LOC)) & (jnp.bitwise_xor(col // E_LOC, me) < jnp.bitwise_xor(row // E_LOC, me)))
    ahead = dot(earlier, got_counts.astype(BF16))
    first = ((row // E_LOC) * SPAN).astype(F32) + start
    kept = jnp.minimum(got_counts, jnp.maximum(capacity - ahead, 0.0))
    last = first + kept
    shift = ((row % E_LOC) * capacity + 1).astype(F32) + ahead - first
    first, last, shift = first[:, 0:1], last[:, 0:1], shift[:, 0:1]
    lane = iota((1, ROWS), 1)
    for c in range(plan.places):
        if c < nc:
            at = trow[:, 0:ROWS] + float(c * Z)
        else:
            at = (jnp.bitwise_xor(lane // Z, 1) * SPAN + (2 * nc * Z - 1 - (nc - 1) * Z) - lane % Z).astype(F32)
        slot = jnp.sum(jnp.where((at >= first) & (at < last), at + shift, 0.0), axis=0, keepdims=True) - 1.0
        dlc[c] = jnp.broadcast_to(slot, (8, ROWS))
        drc[c] = jnp.transpose(jnp.broadcast_to(slot, (128, ROWS)))

    slot_col = iota((slots, 1), 0).astype(F32)
    slot_row = iota((1, plan.wide * slots), 1).astype(F32)

    def pack(c, m):
        mask = drc[c, :, 0:1] == (slot_row + m * float(slots) if isinstance(m, int) else slot_row + (m * slots).astype(F32))
        packed = dot(hot(mask), obuf[pl.ds(m, plan.wide)].reshape(plan.wide * slots, d_model))
        return packed.astype(BF16).reshape(GROUP, Z, d_model)

    def send_back(c, packed):
        for k in range(1, GROUP):
            out_copy(c, k).wait_send()
        send[c] = packed
        for k in range(GROUP - 1, 0, -1):
            back_copy(c, k).start()
        rrecv[c, 0] = send[c, 0]

    @pl.loop(0, SETS)
    def _(g):
        @pl.loop(pick(plan.hi_before, g), pick(plan.hi, g))
        def _(c):
            @pl.when(c < nc)
            def _():
                for k in range(1, GROUP):
                    out_copy(c, k).wait_recv()

            if plan.shared:
                @pl.when(c == nc - 1)
                def _():
                    pass_on().start()

                @pl.when(c == nc)
                def _():
                    pass_on().wait_recv()

        acc[...] = jnp.zeros_like(acc)

        @pl.loop(0, pick(plan.pairs, g))
        def _(p):
            c = pick(plan.hi, g) - 2 * p - 2
            slot = jnp.concatenate([dlc[c, 0:1, :], dlc[c + 1, 0:1, :]], axis=1)
            mask = (slot_col + (g * slots).astype(F32)) == slot
            acc[...] += dot(hot(mask), recv[pl.ds(c, 2)].reshape(2 * ROWS, d_model))

        bbuf[...] = acc[...].astype(BF16)

        @pl.loop(0, PER)
        def _(j):
            at = pl.ds(pl.multiple_of(j * capacity, capacity), capacity)
            first_i = (g * PER + j) * per_e
            total = None
            for f in range(per_e):
                i = first_i + f
                slot = i % ns
                for copy in w_copies(i, slot):
                    copy.wait()
                v = dot(bbuf[at, :], wi[slot])
                u = v * (0.7978845608028654 + (0.7978845608028654 * 0.044715) * (v * v))
                half = 0.5 * v
                part = dot((half + half * jnp.tanh(u)).astype(BF16), wo[slot])
                total = part if total is None else total + part

                @pl.when(i + ns < E_LOC * per_e)
                def _():
                    for copy in w_copies(i + ns, slot):
                        copy.start()
            obuf[g, at, :] = total.astype(BF16)

        @pl.loop(pick(plan.lo, g), pick(plan.lo_next, g))
        def _(c):
            send_back(c, pack(c, pick(plan.first, c)))

    if plan.shared:
        xsend[...] = pack(nc, plan.first[nc])
        hand_over().start()
        packed = pack(nc - 1, plan.first[nc - 1])
        hand_over().wait_recv()
        send_back(nc - 1, packed + xrecv[...])

    def combine(c, count, fresh, finish):
        want = trow[:, 0:count * ROWS] + float(c * Z)
        for m in range(count):
            for k in range(1, GROUP):
                back_copy(c + m, k).wait_recv()

        @pl.loop(0, n_tok // TTILE)
        def _(t):
            at = pl.ds(pl.multiple_of(t * TTILE, TTILE), TTILE)
            rows = rrecv[c:c + count].reshape(count * ROWS, d_model)
            new = dot(hot(qcol[at, 0:1] == want), rows)
            if not fresh:
                new = got[at, :].astype(F32) + new
            if finish:
                new = xv[at, :].astype(F32) + qcol[at, 1:2] * new
            got[at, :] = new.astype(BF16)
            if finish:
                y_copy(t).start()

    c = 0
    for count in plan.batches:
        combine(c, count, c == 0, c + count == sum(plan.batches))
        c += count

    if c < nc:
        for k in range(1, GROUP):
            back_copy(c, k).wait_recv()
    tail_ref[...] = rrecv[nc - 1]

    for k in range(1, GROUP):
        count_copy(k).wait_send()
    if plan.shared:
        pass_on().wait_send()
        hand_over().wait_send()

    @pl.loop(0, nc)
    def _(c):
        for k in range(1, GROUP):
            back_copy(c, k).wait_send()

    flag_copy.wait()
    c_copy.wait()
    for t in range(n_tok // TTILE):
        y_copy(t).wait()


def close_kernel(shift, y1_ref, tail_ref, cols_ref, y_ref):
    i = iota((1, ROWS), 1)
    want = ((i // Z) * (SPAN - Z) + i + shift).astype(F32)
    new = dot(hot(cols_ref[:, 0:1] == want), tail_ref[...])
    y_ref[...] = (y1_ref[...].astype(F32) + cols_ref[:, 1:2] * new).astype(BF16)


def solution(mesh):
    dev_axes = ('ep2', 'ep')

    def local_step(x_loc, ids_loc, gate_loc, w_a, w_b):
        n_tok, d_model = x_loc.shape
        capacity = 8 * ((5 * GROUP * n_tok) // (32 * EXPERTS))
        vmem = pl.BlockSpec(memory_space=pltpu.VMEM)
        hbm = pl.BlockSpec(memory_space=pl.ANY)
        dma = pltpu.SemaphoreType.DMA
        gate_row = gate_loc.reshape(1, n_tok)
        args = (ids_loc.reshape(1, n_tok), gate_row, x_loc, w_a, w_b)

        def moe(plan, number):
            nc, ns = plan.chunks, plan.slots
            block = pltpu.VMEM((nc, GROUP, Z, d_model), BF16)
            chunk = pltpu.VMEM((GROUP, Z, d_model), BF16)
            return pl.pallas_call(
                functools.partial(moe_kernel, plan, capacity),
                out_shape=(jax.ShapeDtypeStruct((n_tok, d_model), BF16), jax.ShapeDtypeStruct((GROUP, Z, d_model), BF16),
                           jax.ShapeDtypeStruct((n_tok, 128), F32), jax.ShapeDtypeStruct((1, 1), F32)),
                in_specs=[hbm] * 5, out_specs=(hbm, vmem, hbm, hbm),
                scratch_shapes=[
                    pltpu.VMEM((1, n_tok), jnp.int32), pltpu.VMEM((1, n_tok), F32), pltpu.SMEM((1, 1), F32),
                    pltpu.VMEM((n_tok, d_model), BF16), pltpu.VMEM((n_tok, d_model), BF16),
                    block, pltpu.VMEM((plan.places, GROUP, Z, d_model), BF16), block, chunk, chunk,
                    pltpu.VMEM((PER * capacity, d_model), BF16), pltpu.VMEM((SETS, PER * capacity, d_model), BF16),
                    pltpu.VMEM((PER * capacity, d_model), F32),
                    pltpu.VMEM((ns, d_model, FTILE), BF16), pltpu.VMEM((ns, FTILE, d_model), BF16),
                    pltpu.VMEM((GROUP, E_LOC + 8, 128), F32), pltpu.VMEM((GROUP, E_LOC + 8, 128), F32),
                    pltpu.VMEM((8, n_tok), F32), pltpu.VMEM((n_tok, 128), F32),
                    pltpu.VMEM((plan.places, 8, ROWS), F32), pltpu.VMEM((plan.places, ROWS, 128), F32),
                    dma((3,)), dma((n_tok // XTILE,)), dma((n_tok // TTILE,)), dma(()), dma((GROUP,)), dma((GROUP,)),
                    dma((nc, GROUP)), dma((nc, GROUP)), dma((nc, GROUP)), dma((nc, GROUP)), dma((2,)), dma((2,)), dma((ns,)), dma((ns,)),
                ],
                compiler_params=pltpu.CompilerParams(
                    collective_id=number, has_side_effects=True, vmem_limit_bytes=66_000_000),
                name='moe_' + str(nc),
            )(*args)

        y1, tail, cols, flag = moe(FAST, 0)
        y1, tail = lax.cond(flag[0, 0] > 0.0, lambda: (moe(SAFE, 1)[0], jnp.zeros_like(tail)), lambda: (y1, tail))
        rows = lambda width: pl.BlockSpec((CTILE, width), lambda t: (t, 0))
        return pl.pallas_call(
            functools.partial(close_kernel, (FAST.chunks - 1) * Z),
            out_shape=jax.ShapeDtypeStruct((n_tok, d_model), BF16), grid=(n_tok // CTILE,),
            in_specs=[rows(d_model), pl.BlockSpec((ROWS, d_model), lambda t: (0, 0)), rows(128)], out_specs=rows(d_model),
            name='close',
        )(y1, tail.reshape(ROWS, d_model), cols)

    tok_spec = P(('dp', 'ep2', 'ep'), None)
    w_spec = P(dev_axes, None, None)
    return jax.shard_map(local_step, mesh=mesh, in_specs=(tok_spec, tok_spec, tok_spec, w_spec, w_spec), out_specs=tok_spec, check_vma=False)
```

```python
import functools

import jax
import jax.numpy as jnp
from jax import lax
from jax.experimental import pallas as pl
from jax.experimental.pallas import tpu as pltpu
from jax.sharding import PartitionSpec as P

MESH = pl.DeviceIdType.MESH
F32 = jnp.float32
BF16 = jnp.bfloat16
GROUP = 8
EXPERTS = 128
E_LOC = EXPERTS // GROUP
SPAN = 512
Z = 32
ROWS = GROUP * Z
PER = 2
SETS = E_LOC // PER
FTILE = 1536
TTILE = 256
XTILE = 2048
CTILE = 1024


def pick(values, i):
    out = values[0]
    for m in range(1, len(values)):
        out = out + (values[m] - values[m - 1]) * ((i + 16 - m) // 16)
    return out


class Plan:
    def __init__(self, lo, hi, slots, batches, shared):
        self.lo, self.hi, self.slots, self.shared = lo, hi, slots, shared
        self.places = hi[-1]
        self.chunks = self.places - shared
        self.batches = batches
        assert sum(batches) in (self.chunks, self.chunks - 1)
        self.hi_before = (0,) + hi[:-1]
        self.lo_next = lo[1:] + (self.chunks - shared,)
        assert all(a <= b for a, b in zip(lo, self.lo_next))
        self.pairs = tuple((h - l + 1) // 2 for l, h in zip(lo, hi))
        first = [min(m for m in range(SETS) if hi[m] > c) for c in range(self.places)]
        after = [max(m for m in range(SETS) if lo[m] <= c) + 1 for c in range(self.places)]
        self.wide = max(b - a for a, b in zip(first, after))
        self.first = tuple(min(m, SETS - self.wide) for m in first)
        assert all(h >= 2 * p for h, p in zip(hi, self.pairs))


FAST = Plan((0, 0, 1, 2, 3, 5, 6, 7), (2, 4, 6, 7, 8, 9, 10, 11), 5, (4, 4, 1), 1)
SAFE = Plan((0,) * 8, (2, 4, 6, 8, 10, 12, 14, 16), 3, (4, 4, 4, 4), 0)


def position():
    ep = lax.axis_index('ep')
    return lax.axis_index('ep2'), ep // 2, ep % 2


def partner(where, k):
    y, x, c = where
    py = (y + k // 4) % 2
    px = (x + (k // 2) % 2) % 2
    pc = (c + k % 2) % 2
    return py * 4 + px * 2 + pc, {'ep2': py, 'ep': px * 2 + pc}


def iota(shape, dim):
    return lax.broadcasted_iota(jnp.int32, shape, dim)


def hot(mask):
    return jnp.where(mask, 1.0, 0.0).astype(BF16)


def dot(a, b):
    return jnp.dot(a, b, preferred_element_type=F32)


def moe_kernel(plan, capacity, ids_hbm, gate_hbm, x_hbm, w_in, w_out, y_hbm, tail_ref, cols_hbm, flag_hbm,
               ids_ref, gate_ref, flag_ref, xv, got, send, recv, rrecv, xsend, xrecv, bbuf, obuf, acc, wi, wo, xbuf, cbuf, qrow, qcol, dlc, drc,
               i_sem, x_sem, y_sem, c_sem, n_send, n_recv, s_send, s_recv, r_send, r_recv, x_send, x_recv, wi_sem, wo_sem):
    nc, ns = plan.chunks, plan.slots
    n_tok, d_model = xv.shape
    per_e = w_in.shape[2] // FTILE
    slots = PER * capacity
    where = position()
    me = partner(where, 0)[0]

    def w_copies(i, slot):
        e, f = i // per_e, i % per_e
        cols = pl.ds(pl.multiple_of(f * FTILE, FTILE), FTILE)
        return (pltpu.make_async_copy(w_in.at[e, :, cols], wi.at[slot], wi_sem.at[slot]),
                pltpu.make_async_copy(w_out.at[e, cols, :], wo.at[slot], wo_sem.at[slot]))

    def x_copy(q):
        at = pl.ds(q * XTILE, XTILE)
        return pltpu.make_async_copy(x_hbm.at[at, :], xv.at[at, :], x_sem.at[q])

    def y_copy(t):
        at = pl.ds(pl.multiple_of(t * TTILE, TTILE), TTILE)
        return pltpu.make_async_copy(got.at[at, :], y_hbm.at[at, :], y_sem.at[t])

    def remote(src, dst, sent, received, k):
        return pltpu.make_async_remote_copy(src_ref=src, dst_ref=dst, send_sem=sent, recv_sem=received,
                                            device_id=partner(where, k)[1], device_id_type=MESH)

    def count_copy(k):
        return remote(xbuf.at[k], cbuf.at[k], n_send.at[k], n_recv.at[k], k)

    def out_copy(c, k):
        return remote(send.at[c, k], recv.at[c, k], s_send.at[c, k], s_recv.at[c, k], k)

    def pass_on():
        return remote(recv.at[nc - 1], recv.at[nc], x_send.at[0], x_recv.at[0], 1)

    def hand_over():
        return remote(xsend, xrecv, x_send.at[1], x_recv.at[1], 1)

    def back_copy(c, k):
        return remote(send.at[c, k], rrecv.at[c, k], r_send.at[c, k], r_recv.at[c, k], k)

    ids_copy = pltpu.make_async_copy(ids_hbm, ids_ref, i_sem.at[0])
    gate_copy = pltpu.make_async_copy(gate_hbm, gate_ref, i_sem.at[1])
    flag_copy = pltpu.make_async_copy(flag_ref, flag_hbm, i_sem.at[2])
    ids_copy.start()
    gate_copy.start()
    barrier = pltpu.get_barrier_semaphore()
    for k in range(1, GROUP):
        pl.semaphore_signal(barrier, inc=1, device_id=partner(where, k)[1], device_id_type=MESH)
    for q in range(n_tok // XTILE):
        x_copy(q).start()

    obuf[...] = jnp.zeros_like(obuf)

    row, col = iota((EXPERTS, EXPERTS), 0), iota((EXPERTS, EXPERTS), 1)
    same = (row // E_LOC) == (col // E_LOC)
    in_row, in_col = (row % E_LOC) // PER, (col % E_LOC) // PER
    inner = hot(same & (in_row == in_col) & (col < row))
    sums = [hot(same & (in_col == g)) for g in range(SETS)]

    def starts(counts):
        counts = counts.astype(BF16)
        base = jnp.zeros((EXPERTS, EXPERTS), F32)
        mine, over = base, base
        for g in range(SETS):
            if g:
                base = jnp.maximum(base, float(plan.lo[g] * Z))
            mine = jnp.where(in_row == g, base, mine)
            base = base + dot(sums[g], counts)
            over = jnp.maximum(over, base - float(plan.hi[g] * Z))
        if plan.shared:
            other = jnp.concatenate([base[(b ^ 1) * E_LOC:((b ^ 1) + 1) * E_LOC] for b in range(GROUP)], axis=0)
            over = jnp.maximum(over, base + other - float(2 * nc * Z))
        return mine + dot(inner, counts), over

    ids_copy.wait()
    chosen = hot(iota((EXPERTS, n_tok), 0) == ids_ref[...])
    counts = dot(chosen, jnp.ones((n_tok, 128), BF16))
    start, over = starts(counts)
    to_k = jnp.bitwise_xor(row // E_LOC, me).astype(F32)
    code0 = to_k * float(SPAN) + start

    upper = hot((iota((TTILE, TTILE + 128), 0) < iota((TTILE, TTILE + 128), 1)) | (iota((TTILE, TTILE + 128), 1) >= TTILE))
    base = code0
    for b in range(n_tok // TTILE):
        part = chosen[:, b * TTILE:(b + 1) * TTILE]
        rank = dot(part, upper)
        full = jnp.concatenate([rank[:, i * 128:(i + 1) * 128] + base for i in range(TTILE // 128)], axis=1)
        code = jnp.sum(part.astype(F32) * full, axis=0, keepdims=True)
        if plan.shared:
            whole = code.astype(jnp.int32)
            k, place = whole // SPAN, whole % SPAN
            mirrored = jnp.bitwise_xor(k, 1) * SPAN + (2 * nc * Z - 1) - place
            code = jnp.where(place >= nc * Z, mirrored, whole).astype(F32)
        qrow[:, b * TTILE:(b + 1) * TTILE] = jnp.broadcast_to(code, (8, TTILE))
        base = base + rank[:, TTILE:]

    worst = jnp.broadcast_to(jnp.max(over, keepdims=True), (8, 128))
    acc[0:EXPERTS, 0:128] = counts
    for k in range(GROUP):
        at = pl.ds(pl.multiple_of(partner(where, k)[0] * E_LOC, E_LOC), E_LOC)
        xbuf[k, 0:E_LOC, :] = acc[at, 0:128]
        xbuf[k, E_LOC:E_LOC + 8, :] = worst
    cbuf[0] = xbuf[0]

    def targets(shape, dim):
        i = iota(shape, dim)
        k = jnp.zeros(shape, jnp.int32)
        c = k
        for m in range(1, -(-shape[dim] // ROWS)):
            c = c + jnp.where(i >= m * ROWS, 1, 0)
        i = i - c * ROWS
        for m in range(1, GROUP):
            k = k + jnp.where(i >= m * Z, 1, 0)
        return (i + k * (SPAN - Z) + c * Z).astype(F32)

    tcol = targets((ROWS, 1), 0)
    trow = targets((1, 4 * ROWS), 1)

    def send_out(c):
        for k in range(GROUP - 1, 0, -1):
            out_copy(c, k).start()
        recv[c, 0] = send[c, 0]

    packed = jnp.zeros((ROWS, d_model), F32)
    for q in range(n_tok // XTILE):
        x_copy(q).wait()
        at = slice(q * XTILE, (q + 1) * XTILE)
        packed = packed + dot(hot(tcol == qrow[0:1, at]), xv[at, :])
    send[0] = packed.astype(BF16).reshape(GROUP, Z, d_model)
    pl.semaphore_wait(barrier, GROUP - 1)
    send_out(0)
    for k in range(1, GROUP):
        count_copy(k).start()

    for i in range(ns):
        for copy in w_copies(i, i):
            copy.start()

    @pl.loop(1, nc)
    def _(c):
        mask = (tcol + (c * Z).astype(F32)) == qrow[0:1, :]
        send[c] = dot(hot(mask), xv[...]).astype(BF16).reshape(GROUP, Z, d_model)
        send_out(c)

    gate_copy.wait()
    for b in range(n_tok // TTILE):
        at = slice(b * TTILE, (b + 1) * TTILE)
        both = jnp.where(iota((128, TTILE), 0) == 0, qrow[0:1, at], gate_ref[0:1, at])
        qcol[at, :] = jnp.transpose(both)
    c_copy = pltpu.make_async_copy(qcol, cols_hbm, c_sem)
    c_copy.start()
    for k in range(1, GROUP):
        count_copy(k).wait_recv()
    flag_ref[0, 0] = jnp.max(cbuf[:, E_LOC:E_LOC + 8, :])
    flag_copy.start()
    got_counts = cbuf[:, 0:E_LOC, :].reshape(EXPERTS, 128)
    start, _ = starts(got_counts)
    earlier = hot(((row % E_LOC) == (col % E_LOC)) & (jnp.bitwise_xor(col // E_LOC, me) < jnp.bitwise_xor(row // E_LOC, me)))
    ahead = dot(earlier, got_counts.astype(BF16))
    first = ((row // E_LOC) * SPAN).astype(F32) + start
    kept = jnp.minimum(got_counts, jnp.maximum(capacity - ahead, 0.0))
    last = first + kept
    shift = ((row % E_LOC) * capacity + 1).astype(F32) + ahead - first
    first, last, shift = first[:, 0:1], last[:, 0:1], shift[:, 0:1]
    lane = iota((1, ROWS), 1)
    for c in range(plan.places):
        if c < nc:
            at = trow[:, 0:ROWS] + float(c * Z)
        else:
            at = (jnp.bitwise_xor(lane // Z, 1) * SPAN + (2 * nc * Z - 1 - (nc - 1) * Z) - lane % Z).astype(F32)
        slot = jnp.sum(jnp.where((at >= first) & (at < last), at + shift, 0.0), axis=0, keepdims=True) - 1.0
        dlc[c] = jnp.broadcast_to(slot, (8, ROWS))
        drc[c] = jnp.transpose(jnp.broadcast_to(slot, (128, ROWS)))

    slot_col = iota((slots, 1), 0).astype(F32)
    slot_row = iota((1, plan.wide * slots), 1).astype(F32)

    def pack(c, m):
        mask = drc[c, :, 0:1] == (slot_row + m * float(slots) if isinstance(m, int) else slot_row + (m * slots).astype(F32))
        packed = dot(hot(mask), obuf[pl.ds(m, plan.wide)].reshape(plan.wide * slots, d_model))
        return packed.astype(BF16).reshape(GROUP, Z, d_model)

    def send_back(c, packed):
        for k in range(1, GROUP):
            out_copy(c, k).wait_send()
        send[c] = packed
        for k in range(GROUP - 1, 0, -1):
            back_copy(c, k).start()
        rrecv[c, 0] = send[c, 0]

    @pl.loop(0, SETS)
    def _(g):
        @pl.loop(pick(plan.hi_before, g), pick(plan.hi, g))
        def _(c):
            @pl.when(c < nc)
            def _():
                for k in range(1, GROUP):
                    out_copy(c, k).wait_recv()

            if plan.shared:
                @pl.when(c == nc - 1)
                def _():
                    pass_on().start()

                @pl.when(c == nc)
                def _():
                    pass_on().wait_recv()

        acc[...] = jnp.zeros_like(acc)

        @pl.loop(0, pick(plan.pairs, g))
        def _(p):
            c = pick(plan.hi, g) - 2 * p - 2
            slot = jnp.concatenate([dlc[c, 0:1, :], dlc[c + 1, 0:1, :]], axis=1)
            mask = (slot_col + (g * slots).astype(F32)) == slot
            acc[...] += dot(hot(mask), recv[pl.ds(c, 2)].reshape(2 * ROWS, d_model))

        bbuf[...] = acc[...].astype(BF16)

        @pl.loop(0, PER)
        def _(j):
            at = pl.ds(pl.multiple_of(j * capacity, capacity), capacity)
            first_i = (g * PER + j) * per_e
            total = None
            for f in range(per_e):
                i = first_i + f
                slot = i % ns
                for copy in w_copies(i, slot):
                    copy.wait()
                v = dot(bbuf[at, :], wi[slot])
                u = v * (0.7978845608028654 + (0.7978845608028654 * 0.044715) * (v * v))
                half = 0.5 * v
                part = dot((half + half * jnp.tanh(u)).astype(BF16), wo[slot])
                total = part if total is None else total + part

                @pl.when(i + ns < E_LOC * per_e)
                def _():
                    for copy in w_copies(i + ns, slot):
                        copy.start()
            obuf[g, at, :] = total.astype(BF16)

        @pl.loop(pick(plan.lo, g), pick(plan.lo_next, g))
        def _(c):
            send_back(c, pack(c, pick(plan.first, c)))

    if plan.shared:
        xsend[...] = pack(nc, plan.first[nc])
        hand_over().start()
        packed = pack(nc - 1, plan.first[nc - 1])
        hand_over().wait_recv()
        send_back(nc - 1, packed + xrecv[...])

    def combine(c, count, fresh, finish):
        want = trow[:, 0:count * ROWS] + float(c * Z)
        for m in range(count):
            for k in range(1, GROUP):
                back_copy(c + m, k).wait_recv()

        @pl.loop(0, n_tok // TTILE)
        def _(t):
            at = pl.ds(pl.multiple_of(t * TTILE, TTILE), TTILE)
            rows = rrecv[c:c + count].reshape(count * ROWS, d_model)
            new = dot(hot(qcol[at, 0:1] == want), rows)
            if not fresh:
                new = got[at, :].astype(F32) + new
            if finish:
                new = xv[at, :].astype(F32) + qcol[at, 1:2] * new
            got[at, :] = new.astype(BF16)
            if finish:
                y_copy(t).start()

    c = 0
    for count in plan.batches:
        combine(c, count, c == 0, c + count == sum(plan.batches))
        c += count

    if c < nc:
        for k in range(1, GROUP):
            back_copy(c, k).wait_recv()
    tail_ref[...] = rrecv[nc - 1]

    for k in range(1, GROUP):
        count_copy(k).wait_send()
    if plan.shared:
        pass_on().wait_send()
        hand_over().wait_send()

    @pl.loop(0, nc)
    def _(c):
        for k in range(1, GROUP):
            back_copy(c, k).wait_send()

    flag_copy.wait()
    c_copy.wait()
    for t in range(n_tok // TTILE):
        y_copy(t).wait()


def close_kernel(shift, y1_ref, tail_ref, cols_ref, y_ref):
    i = iota((1, ROWS), 1)
    want = ((i // Z) * (SPAN - Z) + i + shift).astype(F32)
    new = dot(hot(cols_ref[:, 0:1] == want), tail_ref[...])
    y_ref[...] = (y1_ref[...].astype(F32) + cols_ref[:, 1:2] * new).astype(BF16)


def solution(mesh):
    dev_axes = ('ep2', 'ep')

    def local_step(x_loc, ids_loc, gate_loc, w_a, w_b):
        n_tok, d_model = x_loc.shape
        capacity = 8 * ((5 * GROUP * n_tok) // (32 * EXPERTS))
        vmem = pl.BlockSpec(memory_space=pltpu.VMEM)
        hbm = pl.BlockSpec(memory_space=pl.ANY)
        dma = pltpu.SemaphoreType.DMA
        gate_row = gate_loc.reshape(1, n_tok)
        args = (ids_loc.reshape(1, n_tok), gate_row, x_loc, w_a, w_b)

        def moe(plan, number):
            nc, ns = plan.chunks, plan.slots
            block = pltpu.VMEM((nc, GROUP, Z, d_model), BF16)
            chunk = pltpu.VMEM((GROUP, Z, d_model), BF16)
            return pl.pallas_call(
                functools.partial(moe_kernel, plan, capacity),
                out_shape=(jax.ShapeDtypeStruct((n_tok, d_model), BF16), jax.ShapeDtypeStruct((GROUP, Z, d_model), BF16),
                           jax.ShapeDtypeStruct((n_tok, 128), F32), jax.ShapeDtypeStruct((1, 1), F32)),
                in_specs=[hbm] * 5, out_specs=(hbm, vmem, hbm, hbm),
                scratch_shapes=[
                    pltpu.VMEM((1, n_tok), jnp.int32), pltpu.VMEM((1, n_tok), F32), pltpu.SMEM((1, 1), F32),
                    pltpu.VMEM((n_tok, d_model), BF16), pltpu.VMEM((n_tok, d_model), BF16),
                    block, pltpu.VMEM((plan.places, GROUP, Z, d_model), BF16), block, chunk, chunk,
                    pltpu.VMEM((PER * capacity, d_model), BF16), pltpu.VMEM((SETS, PER * capacity, d_model), BF16),
                    pltpu.VMEM((PER * capacity, d_model), F32),
                    pltpu.VMEM((ns, d_model, FTILE), BF16), pltpu.VMEM((ns, FTILE, d_model), BF16),
                    pltpu.VMEM((GROUP, E_LOC + 8, 128), F32), pltpu.VMEM((GROUP, E_LOC + 8, 128), F32),
                    pltpu.VMEM((8, n_tok), F32), pltpu.VMEM((n_tok, 128), F32),
                    pltpu.VMEM((plan.places, 8, ROWS), F32), pltpu.VMEM((plan.places, ROWS, 128), F32),
                    dma((3,)), dma((n_tok // XTILE,)), dma((n_tok // TTILE,)), dma(()), dma((GROUP,)), dma((GROUP,)),
                    dma((nc, GROUP)), dma((nc, GROUP)), dma((nc, GROUP)), dma((nc, GROUP)), dma((2,)), dma((2,)), dma((ns,)), dma((ns,)),
                ],
                compiler_params=pltpu.CompilerParams(
                    collective_id=number, has_side_effects=True, vmem_limit_bytes=66_000_000),
                name='moe_' + str(nc),
            )(*args)

        y1, tail, cols, flag = moe(FAST, 0)
        y1, tail = lax.cond(flag[0, 0] > 0.0, lambda: (moe(SAFE, 1)[0], jnp.zeros_like(tail)), lambda: (y1, tail))
        rows = lambda width: pl.BlockSpec((CTILE, width), lambda t: (t, 0))
        return pl.pallas_call(
            functools.partial(close_kernel, (FAST.chunks - 1) * Z),
            out_shape=jax.ShapeDtypeStruct((n_tok, d_model), BF16), grid=(n_tok // CTILE,),
            in_specs=[rows(d_model), pl.BlockSpec((ROWS, d_model), lambda t: (0, 0)), rows(128)], out_specs=rows(d_model),
            name='close',
        )(y1, tail.reshape(ROWS, d_model), cols)

    tok_spec = P(('dp', 'ep2', 'ep'), None)
    w_spec = P(dev_axes, None, None)
    return jax.shard_map(local_step, mesh=mesh, in_specs=(tok_spec, tok_spec, tok_spec, w_spec, w_spec), out_specs=tok_spec, check_vma=False)
```
